256 devices in a mesh: fov: 64 (over x, z, y_lo), row: 4 (over y_hi, core).
Axes of the slice: x: 4, y: 4 (y_hi: 2, y_lo: 2; y = y_hi * 2 + y_lo), z: 8, core: 2. Of those that a mesh axis runs over, the one named last changes fastest.
Arguments:
- frames: bfloat16 [64, 5, 512, 512], P('fov', None, 'row'), parts along dimension 0, may hold values from 0.01 to 13, as said below
- phase_offset: float32 [64], P('fov'), parts along dimension 0, may hold values from -3.140625 to 3.140625
- order_gain: float32 [64, 5], P('fov'), parts along dimension 0, may hold values from 0.5 to 2
- band_shift: int32 [64, 2], P('fov'), parts along dimension 0, may hold values from -96 to 96
Outputs:
- picture: float32 [65536, 1024], P(('fov', 'row')), parts along dimension 0
The draws below stay inside these ranges and needn't reach their ends.
There are 64 independent parts, one for each index of `fov`. The reference program is written for one: setup_inputs(seed, part) draws one part's arguments, and reference() takes and returns one part's arrays. A program takes and returns all parts, laid end to end along the dimension named above; each array names one. Nothing has to cross between parts.
Inputs may be any that keep to these rules, and one draw needn't show every extreme that they name: `frames`: positive intensities. `band_shift`: offsets in frequency bins of the 1024-point grid, row component first.
All inputs are finite; a program needn't handle non-finite values.
Results may differ from the reference program's by a relative error of at most 0.0003.
Values sent between devices are 32-bit elements; how exact they have to be, the bound alone decides.
No kernel may reach another device: no remote copies, remote signals or barrier semaphores. Data moves between devices by JAX's collectives and lax.ppermute only.
A program may use at most 128 MiB of HBM per device.

```python
import math
import jax
import jax.numpy as jnp
from jax import lax

PIX = 512
GRID = 1024
PHASES = 5
ANGLES = 1


def draw_frames(key, part):
    subkeys = jax.random.split(key, 4)
    frame_shape = (ANGLES, PHASES, PIX, PIX)
    levels = jax.random.uniform(subkeys[0], (ANGLES, PHASES, 1, 1), jnp.float32, 0.5, 2.0)
    slopes = jax.random.uniform(subkeys[1], (ANGLES, PHASES, 1, 1), jnp.float32, 0.6, 1.2)
    signs_draw = jnp.where(jax.random.bernoulli(subkeys[2], 0.5, (ANGLES, PHASES, 1, 1)), 1.0, -1.0)
    row_pos = (jnp.arange(PIX, dtype=jnp.float32) / PIX - 0.5).reshape(1, 1, PIX, 1)
    profile = jnp.exp(2.0 * slopes * signs_draw * row_pos)
    texture = jnp.clip(1.0 + 0.3 * jax.random.normal(subkeys[3], frame_shape, jnp.float32), 0.1, 1.9)
    return (levels * profile * texture).astype(jnp.bfloat16)


def setup_inputs(seed: int = 0, part: int = 0) -> dict:
    seeds = jax.random.split(jax.random.key(seed), 5)
    own_keys = jax.random.split(jax.random.fold_in(seeds[4], part), 5)
    frames = draw_frames(jax.random.fold_in(jax.random.fold_in(seeds[4], part), 71), part)
    phase_offset = jnp.clip(jax.random.uniform(own_keys[1], (ANGLES,), jnp.float32, -3.140625, 3.140625), -3.140625, 3.140625)
    order_gain = jnp.clip(jnp.exp(jax.random.uniform(own_keys[2], (ANGLES, PHASES), jnp.float32, math.log(0.5), math.log(2.0))), 0.5, 2.0)
    band_shift = jax.random.randint(own_keys[3], (ANGLES, 2), -(3 * PIX) // 16, (3 * PIX) // 16 + 1).astype(jnp.int32)
    return {"frames": frames, "phase_offset": phase_offset, "order_gain": order_gain, "band_shift": band_shift}


wiener = 0.1
gain_out = 8.0
cut_share = 0.45

def wrap_signed(values, length):
    return (values + length // 2) % length - length // 2

def transfer_curve(freq_y, freq_x, cutoff):
    float_y = freq_y.astype(jnp.float32)
    float_x = freq_x.astype(jnp.float32)
    radius = jnp.sqrt(float_y * float_y + float_x * float_x) / cutoff
    radius = jnp.minimum(radius, 1.0)
    return 2.0 / math.pi * (jnp.arccos(radius) - radius * jnp.sqrt(1.0 - radius * radius))

def reference(frames, phase_offset, order_gain, band_shift):
    intensity = frames.astype(jnp.float32)
    totals = lax.optimization_barrier(jnp.sum(intensity, axis=(2, 3)))
    scales = PIX * PIX / totals
    half_pix = PIX // 2
    cutoff = cut_share * PIX
    signed_index = wrap_signed(jnp.arange(PIX, dtype=jnp.int32), PIX)
    base_curve = transfer_curve(signed_index[:, None], signed_index[None, :], cutoff)
    fine_index = jnp.arange(GRID, dtype=jnp.int32)
    numerator = None
    denominator = jnp.full((GRID, GRID), wiener, jnp.float32)
    for angle_idx in range(ANGLES):
        phase_angle = 2.0 * math.pi * jnp.arange(PHASES, dtype=jnp.float32) / PHASES + phase_offset[angle_idx]
        weight = scales[angle_idx] / PHASES
        shift_y = band_shift[angle_idx, 0]
        shift_x = band_shift[angle_idx, 1]
        for order_idx in range(PHASES):
            order_val = order_idx - PHASES // 2
            coef_re = weight * jnp.cos(order_val * phase_angle)
            coef_im = -weight * jnp.sin(order_val * phase_angle)
            band_re = jnp.tensordot(coef_re, intensity[angle_idx], axes=1, precision=lax.Precision.HIGHEST)
            band_im = jnp.tensordot(coef_im, intensity[angle_idx], axes=1, precision=lax.Precision.HIGHEST)
            gain_val = order_gain[angle_idx, order_idx]
            spectrum = jnp.fft.fft2(lax.complex(band_re, band_im)) * (gain_val * base_curve)
            zero_block = jnp.zeros_like(spectrum)
            tall = jnp.concatenate([spectrum[:half_pix], zero_block, spectrum[half_pix:]], axis=0)
            zero_wide = jnp.zeros_like(tall)
            embedded = jnp.concatenate([tall[:, :half_pix], zero_wide, tall[:, half_pix:]], axis=1)
            moved = jnp.roll(jnp.roll(embedded, order_val * shift_y, axis=0), order_val * shift_x, axis=1)
            numerator = moved if numerator is None else numerator + moved
            shifted_curve = transfer_curve(wrap_signed(fine_index[:, None] - order_val * shift_y, GRID), wrap_signed(fine_index[None, :] - order_val * shift_x, GRID), cutoff)
            denominator = denominator + gain_val * gain_val * shifted_curve * shifted_curve
    picture = jnp.fft.ifft2(numerator / denominator)
    return (gain_out * jnp.real(picture)).astype(jnp.float32)
```

```python
import functools
import math

import jax
import jax.numpy as jnp
import numpy as np
from jax import lax
from jax.experimental import pallas as pl
from jax.experimental.pallas import tpu as pltpu
from jax.sharding import PartitionSpec as P

wiener = 0.1
gain_out = 8.0
cut_share = 0.45
PIX = 512
GRID = 1024
PHASES = 5
PARTS = 4
ROWS = PIX // PARTS
MAIN = 64
FOLD = 48
COLS = MAIN + FOLD
EXT = 72


def split_np(array):
    hi = array.astype(jnp.bfloat16)
    lo = (array - hi.astype(np.float32)).astype(jnp.bfloat16)
    return hi, lo


def split(array):
    hi = array.astype(jnp.bfloat16)
    lo = (array - hi.astype(jnp.float32)).astype(jnp.bfloat16)
    return hi, lo


@functools.cache
def tables():
    index = np.arange(PIX)
    angle = 2.0 * np.pi * (np.outer(index, index) % PIX) / PIX
    cos_all = np.cos(angle).astype(np.float32)
    sin_all = np.sin(angle).astype(np.float32)
    sin_half = sin_all[: PIX // 2].copy()
    sin_half[0] = cos_all[PIX // 2]
    x_table = np.stack(
        [np.concatenate([cos_all[d : PIX // 2 : PARTS], sin_half[d::PARTS]]) for d in range(PARTS)]
    )
    y_table = np.stack(
        [
            np.stack([cos_all[s * ROWS : (s + 1) * ROWS], sin_all[s * ROWS : (s + 1) * ROWS]])
            for s in range(PARTS)
        ]
    )
    first = np.zeros((PARTS, 2, COLS, 128), np.float32)
    step = np.zeros((PARTS, 2, COLS, 128), np.float32)
    for s in range(PARTS):
        freq = column_freq_np(s)
        scale = gain_out / (GRID * GRID) * np.where(freq == 0, 1.0, 2.0)
        turn = 2.0 * np.pi * ((freq[:, None] * np.arange(128)[None, :]) % GRID) / GRID
        first[s, 0] = scale[:, None] * np.cos(turn)
        first[s, 1] = scale[:, None] * np.sin(turn)
        turn = 2.0 * np.pi * (freq % 8) / 8
        step[s, 0] = np.cos(turn)[:, None]
        step[s, 1] = np.sin(turn)[:, None]
    turn = 2.0 * np.pi * index / GRID
    odd = np.stack([np.cos(turn), np.sin(turn)]).astype(np.float32)
    return split_np(x_table), split_np(y_table), first, step, odd


def column_freq_np(d):
    main = 4 * np.arange(MAIN) + d
    fold = 4 * np.arange(16, 64) + d - PIX
    if d == 0:
        fold[0] = -PIX // 2
    return np.concatenate([main, fold])


def dot3(left, right, dims):
    lhs = jnp.concatenate([left[0], left[0], left[1]], axis=dims[0])
    rhs = jnp.concatenate([right[0], right[1], right[0]], axis=dims[1])
    return lax.dot_general(
        lhs, rhs, (((dims[0],), (dims[1],)), ((), ())), preferred_element_type=jnp.float32
    )


def turn_pair(steps):
    angle = (2.0 * math.pi / PIX) * ((steps + 256) % 512 - 256).astype(jnp.float32)
    return jnp.cos(angle), jnp.sin(angle)


def forward_kernel(place, shift, offset, totals, frames, x_hi, x_lo, *outs):
    rank = place[0]
    shift_y = shift[0, 0]
    shift_x = shift[0, 1]
    x_cos, x_sin = turn_pair(lax.broadcasted_iota(jnp.int32, (8, PIX), 1) * shift_x)
    row_at = lax.broadcasted_iota(jnp.int32, (ROWS, 128), 0) + rank * ROWS
    y_cos, y_sin = turn_pair(row_at * shift_y)
    x_cos, x_sin = x_cos[:1], x_sin[:1]
    y_cos, y_sin = y_cos[:, :1], y_sin[:, :1]
    turn_re = x_cos * y_cos - x_sin * y_sin
    turn_im = x_cos * y_sin + x_sin * y_cos
    twice_re = turn_re * turn_re - turn_im * turn_im
    twice_im = 2.0 * turn_re * turn_im
    phase_at = lax.broadcasted_iota(jnp.int32, (8, 128), 0).astype(jnp.float32)
    phase_at = (2.0 * math.pi / PHASES) * phase_at + offset[0]
    cos_one, sin_one = jnp.cos(phase_at), jnp.sin(phase_at)
    cos_two, sin_two = jnp.cos(2.0 * phase_at), jnp.sin(2.0 * phase_at)
    sums = [None] * 5
    for p in range(PHASES):
        weight = (PIX * PIX / PHASES) / jnp.full((1, 1), totals[0, p], jnp.float32)
        plane = weight * frames[0, p].astype(jnp.float32)
        at = (slice(p, p + 1), slice(0, 1))
        terms = [
            plane,
            plane * cos_one[at],
            plane * sin_one[at],
            plane * cos_two[at],
            plane * sin_two[at],
        ]
        sums = terms if p == 0 else [a + b for a, b in zip(sums, terms)]
    zero, one_re, one_im, two_re, two_im = sums
    planes = [
        zero,
        one_re * turn_re + one_im * turn_im,
        one_re * turn_im - one_im * turn_re,
        two_re * twice_re + two_im * twice_im,
        two_re * twice_im - two_im * twice_re,
    ]
    band = split(jnp.concatenate(planes, axis=0))
    table = (
        jnp.concatenate([x_hi[rank ^ k] for k in range(PARTS)], axis=0),
        jnp.concatenate([x_lo[rank ^ k] for k in range(PARTS)], axis=0),
    )
    spectra = dot3(table, band, (1, 1))
    for k in range(PARTS):
        for plane in range(5):
            outs[k][plane] = spectra[k * 128 : (k + 1) * 128, plane * ROWS : (plane + 1) * ROWS]


def middle_kernel(place, got0, got1, got2, got3, weights, y_hi, y_lo, odd, *outs):
    rank = place[0]
    blocks = (got0, got1, got2, got3)
    first_row = lax.broadcasted_iota(jnp.int32, (MAIN, PIX), 0) == 0
    lone = jnp.logical_and(first_row, jnp.full((MAIN, PIX), rank, jnp.int32) == 0)
    top = lax.broadcasted_iota(jnp.int32, (EXT - MAIN, PIX), 0) == 0

    def plane(index):
        whole = jnp.concatenate([b[index] for b in blocks], axis=1)
        sines = whole[MAIN:]
        extra = jnp.where(top, sines[: EXT - MAIN], 0.0)
        return whole[:MAIN], jnp.where(lone, 0.0, sines), extra

    real_rows = []
    imag_rows = []
    cos_r, sin_r, extra_r = plane(0)
    real_rows += [cos_r, extra_r]
    imag_rows += [-sin_r, jnp.zeros_like(extra_r)]
    for m in range(2):
        cos_r, sin_r, extra_r = plane(1 + 2 * m)
        cos_i, sin_i, extra_i = plane(2 + 2 * m)
        real_rows += [cos_r + sin_i, extra_r, cos_r - sin_i, extra_r]
        imag_rows += [cos_i - sin_r, extra_i, -cos_i - sin_r, -extra_i]
    data = split(jnp.concatenate(real_rows + imag_rows, axis=0))

    def y_block(ref, k, part):
        return ref[rank ^ k, part]

    def y_matrix(ref):
        return jnp.concatenate(
            [
                jnp.concatenate([y_block(ref, k, 0), y_block(ref, k, 1)], axis=1)
                for k in range(PARTS)
            ],
            axis=0,
        )

    turned = dot3(data, (y_matrix(y_hi), y_matrix(y_lo)), (1, 0))
    half = 5 * EXT
    spec_re = turned[:half, :PIX] + turned[half:, PIX:]
    spec_im = turned[half:, :PIX] - turned[:half, PIX:]
    even_re = even_im = odd_re = odd_im = None
    tile_top = lax.broadcasted_iota(jnp.int32, (8, PIX), 0) == 0
    for order in range(5):
        def rows(spec):
            main = spec[order * EXT : order * EXT + MAIN]
            extra = spec[order * EXT + MAIN : (order + 1) * EXT]
            tile = jnp.where(tile_top, extra, main[16:24])
            return jnp.concatenate([main, tile, main[24:]], axis=0)

        re, im = rows(spec_re), rows(spec_im)
        plus, minus = weights[order, 0], weights[order, 1]
        terms = (plus * re, plus * im, minus * re, minus * im)
        if order == 0:
            even_re, even_im, odd_re, odd_im = terms
        else:
            even_re, even_im = even_re + terms[0], even_im + terms[1]
            odd_re, odd_im = odd_re + terms[2], odd_im + terms[3]
    odd_cos, odd_sin = odd[0:1], odd[1:2]
    odd_re, odd_im = odd_re * odd_cos - odd_im * odd_sin, odd_re * odd_sin + odd_im * odd_cos
    filtered = split(jnp.concatenate([even_re, even_im, odd_re, odd_im], axis=0))

    def u_matrix(ref):
        return jnp.concatenate(
            [
                jnp.concatenate([y_block(ref, k, 0), y_block(ref, k, 1)], axis=0)
                for k in range(PARTS)
            ],
            axis=0,
        )

    back = dot3(filtered, (u_matrix(y_hi), u_matrix(y_lo)), (1, 1))
    for k in range(PARTS):
        cos_part = back[:, 2 * ROWS * k : 2 * ROWS * k + ROWS]
        sin_part = back[:, 2 * ROWS * k + ROWS : 2 * ROWS * (k + 1)]
        for parity in range(2):
            base = 2 * COLS * parity
            re, im = slice(base, base + COLS), slice(base + COLS, base + 2 * COLS)
            outs[k][0:COLS, parity * ROWS : (parity + 1) * ROWS] = cos_part[re] - sin_part[im]
            outs[k][COLS : 2 * COLS, parity * ROWS : (parity + 1) * ROWS] = (
                sin_part[re] + cos_part[im]
            )


def final_kernel(place, got0, got1, got2, got3, first, step, out, woven):
    rank = place[0]
    blocks = (got0, got1, got2, got3)
    table_rows = []
    for k in range(PARTS):
        source = rank ^ k
        re, im = first[source, 0], first[source, 1]
        step_re, step_im = step[source, 0], step[source, 1]
        res, ims = [re], [-im]
        for _ in range(7):
            re, im = re * step_re - im * step_im, re * step_im + im * step_re
            res.append(re)
            ims.append(-im)
        table_rows += [jnp.concatenate(res, axis=1), jnp.concatenate(ims, axis=1)]
    table = split(jnp.concatenate(table_rows, axis=0))
    data = split(jnp.concatenate([b[...] for b in blocks], axis=0))
    picture = dot3(data, table, (0, 0))
    for block in range(GRID // 128):
        lanes = slice(128 * block, 128 * (block + 1))
        woven[block, pl.ds(0, ROWS, 2), :] = picture[:ROWS, lanes]
        woven[block, pl.ds(1, ROWS, 2), :] = picture[ROWS:, lanes]
        out[:, lanes] = woven[block]


def order_weights(rank, gains, shift):
    cutoff = cut_share * PIX
    row = jnp.arange(COLS, dtype=jnp.int32)
    freq_x = jnp.where(row < MAIN, 4 * row + rank, 4 * (row - FOLD) + rank - PIX)
    freq_x = jnp.where((row == MAIN) & (rank == 0), -PIX // 2, freq_x)
    freq_y = (
        jnp.arange(PIX, dtype=jnp.int32)[None, :] - PIX * jnp.arange(2, dtype=jnp.int32)[:, None]
    )
    curves = []
    for m in (0, 1, -1, 2, -2):
        x = (freq_x - m * shift[1]).astype(jnp.float32)[None, :, None]
        y = (freq_y - m * shift[0]).astype(jnp.float32)[:, None, :]
        radius = jnp.minimum(jnp.sqrt(y * y + x * x) / cutoff, 1.0)
        curves.append(
            2.0 / math.pi * (jnp.arccos(radius) - radius * jnp.sqrt(1.0 - radius * radius))
        )
    own = [gains[2], gains[3], gains[1], gains[4], gains[0]]
    other = [gains[2], gains[1], gains[3], gains[0], gains[4]]
    own_den = wiener + sum(g * g * c * c for g, c in zip(own, curves))
    other_den = wiener + sum(g * g * c * c for g, c in zip(other, curves))
    own_den = 0.5 / own_den
    other_den = 0.5 / other_den
    result = []
    for g, h, c in zip(own, other, curves):
        weight = c * (g * own_den + h * other_den)
        result.append(jnp.stack([weight[0] + weight[1], weight[0] - weight[1]]))
    return jnp.stack(result)


def smem():
    return pl.BlockSpec(memory_space=pltpu.SMEM)


def vmem():
    return pl.BlockSpec(memory_space=pltpu.VMEM)


def from_partners(blocks):
    got = [blocks[0]]
    for k in range(1, PARTS):
        got.append(lax.ppermute(blocks[k], "row", [(i, i ^ k) for i in range(PARTS)]))
    return got


def per_device(frames, phase_offset, order_gain, band_shift):
    (x_hi, x_lo), (y_hi, y_lo), first, step, odd = tables()
    rank = lax.axis_index("row")
    place = rank.reshape(1).astype(jnp.int32)
    totals = lax.psum(jnp.sum(frames.astype(jnp.float32), axis=(2, 3)), "row")
    params = pltpu.CompilerParams(vmem_limit_bytes=40 * 1024 * 1024)
    sent = pl.pallas_call(
        forward_kernel,
        out_shape=[jax.ShapeDtypeStruct((5, 128, ROWS), jnp.float32)] * PARTS,
        in_specs=[smem()] * 4 + [vmem()] * 3,
        out_specs=[vmem()] * PARTS,
        compiler_params=params,
    )(place, band_shift, phase_offset, totals, frames, x_hi, x_lo)
    got = from_partners(sent)
    weights = order_weights(rank, order_gain[0], band_shift[0])
    sent = pl.pallas_call(
        middle_kernel,
        out_shape=[jax.ShapeDtypeStruct((2 * COLS, 2 * ROWS), jnp.float32)] * PARTS,
        in_specs=[smem()] + [vmem()] * 8,
        out_specs=[vmem()] * PARTS,
        compiler_params=params,
    )(place, *got, weights, y_hi, y_lo, odd)
    got = from_partners(sent)
    return pl.pallas_call(
        final_kernel,
        out_shape=jax.ShapeDtypeStruct((2 * ROWS, GRID), jnp.float32),
        in_specs=[smem()] + [vmem()] * 6,
        out_specs=vmem(),
        scratch_shapes=[pltpu.VMEM((GRID // 128, 2 * ROWS, 128), jnp.float32)],
        compiler_params=params,
    )(place, *got, first, step)


def solution(mesh):
    in_specs = (P("fov", None, "row", None), P("fov"), P("fov", None), P("fov", None))
    out_specs = P(("fov", "row"), None)
    return jax.shard_map(
        per_device, mesh=mesh, in_specs=in_specs, out_specs=out_specs, check_vma=False
    )
```

```python
import functools
import math

import jax
import jax.numpy as jnp
import numpy as np
from jax import lax
from jax.experimental import pallas as pl
from jax.experimental.pallas import tpu as pltpu
from jax.sharding import PartitionSpec as P

wiener = 0.1
gain_out = 8.0
cut_share = 0.45
PIX = 512
GRID = 1024
PHASES = 5
PARTS = 4
ROWS = PIX // PARTS
CHUNKS = (0, 1)
LOW = (32, 0)
MAIN = 32
FOLD_LOW = (32, 16)
FOLD = (32, 16)
COLS = (64, 48)
EXT = (32, 40)
ORDERS = (0, 1, -1, 2, -2)
ARC = (
    1.5707963050,
    -0.2145988016,
    0.0889789874,
    -0.0501743046,
    0.0308918810,
    -0.0170881256,
    0.0066700901,
    -0.0012624911,
)


def split_np(array):
    hi = array.astype(jnp.bfloat16)
    lo = (array - hi.astype(np.float32)).astype(jnp.bfloat16)
    return hi, lo


def split(array):
    hi = array.astype(jnp.bfloat16)
    lo = (array - hi.astype(jnp.float32)).astype(jnp.bfloat16)
    return hi, lo


def column_freq_np(d, chunk):
    main = 4 * (np.arange(MAIN) + LOW[chunk]) + d
    fold = 4 * (np.arange(FOLD[chunk]) + FOLD_LOW[chunk]) + d - PIX
    if d == 0 and chunk == 1:
        fold[0] = -PIX // 2
    return np.concatenate([main, fold])


@functools.cache
def tables():
    index = np.arange(PIX)
    angle = 2.0 * np.pi * (np.outer(index, index) % PIX) / PIX
    cos_all = np.cos(angle).astype(np.float32)
    sin_all = np.sin(angle).astype(np.float32)
    sin_half = sin_all[: PIX // 2].copy()
    sin_half[0] = cos_all[PIX // 2]
    x_table = np.stack(
        [
            np.stack(
                [
                    np.concatenate(
                        [
                            cos_all[d : PIX // 2 : PARTS][LOW[c] : LOW[c] + MAIN],
                            sin_half[d::PARTS][LOW[c] : LOW[c] + MAIN],
                        ]
                    )
                    for d in range(PARTS)
                ]
            )
            for c in CHUNKS
        ]
    )
    y_table = np.stack(
        [
            np.stack([cos_all[s * ROWS : (s + 1) * ROWS], sin_all[s * ROWS : (s + 1) * ROWS]])
            for s in range(PARTS)
        ]
    )
    first = []
    for c in CHUNKS:
        block = np.zeros((PARTS, 2, COLS[c], 128), np.float32)
        for s in range(PARTS):
            freq = column_freq_np(s, c)
            scale = gain_out / (GRID * GRID) * np.where(freq == 0, 1.0, 2.0)
            turn = 2.0 * np.pi * ((freq[:, None] * np.arange(128)[None, :]) % GRID) / GRID
            block[s, 0] = scale[:, None] * np.cos(turn)
            block[s, 1] = scale[:, None] * np.sin(turn)
        first.append(block)
    turn = 2.0 * np.pi * index / GRID
    odd = np.stack([np.cos(turn), np.sin(turn)]).astype(np.float32)
    return split_np(x_table), split_np(y_table), first, odd


def dot3(left, right, dims):
    lhs = jnp.concatenate([left[0], left[0], left[1]], axis=dims[0])
    rhs = jnp.concatenate([right[0], right[1], right[0]], axis=dims[1])
    return lax.dot_general(
        lhs, rhs, (((dims[0],), (dims[1],)), ((), ())), preferred_element_type=jnp.float32
    )


def turn_pair(steps):
    angle = (2.0 * math.pi / PIX) * ((steps + 256) % 512 - 256).astype(jnp.float32)
    return jnp.cos(angle), jnp.sin(angle)


def sums_kernel(source, sums, frames, sems):
    copies = [
        pltpu.make_async_copy(source.at[0, p], frames.at[p], sems.at[p]) for p in range(PHASES)
    ]
    for copy in copies:
        copy.start()
    for p in range(PHASES):
        copies[p].wait()
        rows = jnp.sum(frames[p].astype(jnp.float32), axis=0, keepdims=True)
        lanes = rows[:, :128] + rows[:, 128:256] + rows[:, 256:384] + rows[:, 384:]
        sums[p : p + 1, :] = lanes
    sums[PHASES:, :] = jnp.zeros((8 - PHASES, 128), jnp.float32)


def phase_kernel(place, shift, offset, hi_any, lo_any, turns, phases, x_hi, x_lo, sems):
    copies = [
        pltpu.make_async_copy(hi_any, x_hi, sems.at[0]),
        pltpu.make_async_copy(lo_any, x_lo, sems.at[1]),
    ]
    for copy in copies:
        copy.start()
    rank = place[0]
    shift_y = shift[0, 0]
    shift_x = shift[0, 1]
    x_cos, x_sin = turn_pair(lax.broadcasted_iota(jnp.int32, (8, PIX), 1) * shift_x)
    row_at = lax.broadcasted_iota(jnp.int32, (ROWS, 128), 0) + rank * ROWS
    y_cos, y_sin = turn_pair(row_at * shift_y)
    x_cos, x_sin = x_cos[:1], x_sin[:1]
    y_cos = jnp.concatenate([y_cos] * 4, axis=1)
    y_sin = jnp.concatenate([y_sin] * 4, axis=1)
    turn_re = x_cos * y_cos - x_sin * y_sin
    turn_im = x_cos * y_sin + x_sin * y_cos
    turns[0] = turn_re
    turns[1] = turn_im
    turns[2] = turn_re * turn_re - turn_im * turn_im
    turns[3] = 2.0 * turn_re * turn_im
    phase_at = lax.broadcasted_iota(jnp.int32, (8, 128), 0).astype(jnp.float32)
    phase_at = (2.0 * math.pi / PHASES) * phase_at + offset[0]
    phases[0] = jnp.cos(phase_at)
    phases[1] = jnp.sin(phase_at)
    phases[2] = jnp.cos(2.0 * phase_at)
    phases[3] = jnp.sin(2.0 * phase_at)
    for copy in copies:
        copy.wait()


def spectra_rows(rank, chunk, band, x_hi, x_lo, outs):
    table = (
        jnp.concatenate([x_hi[chunk, rank ^ k] for k in range(PARTS)], axis=0),
        jnp.concatenate([x_lo[chunk, rank ^ k] for k in range(PARTS)], axis=0),
    )
    spectra = dot3(table, band, (1, 1))
    for k in range(PARTS):
        for plane in range(5):
            outs[k][plane] = spectra[
                k * 2 * MAIN : (k + 1) * 2 * MAIN, plane * ROWS : (plane + 1) * ROWS
            ]


def forward_kernel(place, sums0, sums1, sums2, sums3, turns, phases, frames, x_hi, x_lo, *rest):
    outs, (band_hi, band_lo) = rest[:PARTS], rest[PARTS:]
    rank = place[0]
    total = (sums0[...] + sums1[...]) + (sums2[...] + sums3[...])
    total = jnp.sum(total, axis=1, keepdims=True)
    weight_all = (PIX * PIX / PHASES) / total[:PHASES]
    acc = None
    for p in range(PHASES):
        weight = weight_all[p : p + 1]
        plane = frames[p].astype(jnp.float32)
        terms = [plane * weight] + [
            plane * (weight * phases[i, p : p + 1, 0:1]) for i in range(4)
        ]
        acc = terms if p == 0 else [a + b for a, b in zip(acc, terms)]
    zero, one_re, one_im, two_re, two_im = acc
    planes = [
        zero,
        one_re * turns[0] + one_im * turns[1],
        one_re * turns[1] - one_im * turns[0],
        two_re * turns[2] + two_im * turns[3],
        two_re * turns[3] - two_im * turns[2],
    ]
    for index, plane in enumerate(planes):
        hi, lo = split(plane)
        band_hi[index * ROWS : (index + 1) * ROWS, :] = hi
        band_lo[index * ROWS : (index + 1) * ROWS, :] = lo
    spectra_rows(rank, 0, (band_hi[...], band_lo[...]), x_hi, x_lo, outs)


def forward_rest_kernel(place, band_hi, band_lo, x_hi, x_lo, *rest):
    outs, token = rest[:PARTS], rest[PARTS]
    spectra_rows(place[0], 1, (band_hi[...], band_lo[...]), x_hi, x_lo, outs)
    token[...] = jnp.zeros((8, 128), jnp.float32)


def transfer_curve(squared):
    radius = jnp.minimum(jnp.sqrt(squared * (1.0 / (cut_share * PIX) ** 2)), 1.0)
    arc = jnp.full_like(radius, ARC[7])
    for coefficient in ARC[6::-1]:
        arc = arc * radius + coefficient
    return (2.0 / math.pi) * jnp.sqrt(1.0 - radius) * (arc - radius * jnp.sqrt(1.0 + radius))


def weights_kernel(place, gains, shift, token, first0, first1, hi_any, lo_any, *rest):
    weights, final_hi, final_lo = rest[0:2], rest[2:4], rest[4:6]
    y_hi_out, y_lo_out, sems = rest[6:]
    copies = [
        pltpu.make_async_copy(hi_any, y_hi_out, sems.at[0]),
        pltpu.make_async_copy(lo_any, y_lo_out, sems.at[1]),
    ]
    for copy in copies:
        copy.start()
    rank = place[0]
    shift_y, shift_x = shift[0, 0], shift[0, 1]
    own = [gains[0, m + 2] for m in ORDERS]
    other = [gains[0, 2 - m] for m in ORDERS]
    sub = lax.broadcasted_iota(jnp.int32, (8, 1), 0)
    lane = lax.broadcasted_iota(jnp.int32, (1, PIX), 1)

    def tile_step(chunk, tile):
        low = 8 * tile
        folded = low >= MAIN
        freq = 4 * jnp.where(folded, low - MAIN + FOLD_LOW[chunk], low + LOW[chunk]) + rank
        freq = jnp.where(folded, freq - PIX, freq)
        freq_x = freq + 4 * sub
        if chunk == 1:
            lone = jnp.logical_and(low == MAIN, rank == 0)
            freq_x = jnp.where(jnp.where(sub == 0, lone.astype(jnp.int32), 0) == 1, -PIX // 2, freq_x)
        halves = []
        for half in range(2):
            own_den = jnp.full((8, PIX), wiener, jnp.float32)
            other_den = jnp.full((8, PIX), wiener, jnp.float32)
            curves = []
            for m, g, h in zip(ORDERS, own, other):
                x = (freq_x - m * shift_x).astype(jnp.float32)
                y = (lane - (PIX * half + m * shift_y)).astype(jnp.float32)
                curve = transfer_curve(x * x + y * y)
                power = curve * curve
                own_den = own_den + (g * g) * power
                other_den = other_den + (h * h) * power
                curves.append(curve)
            own_den = 0.5 / own_den
            other_den = 0.5 / other_den
            halves.append([c * (g * own_den + h * other_den) for c, g, h in zip(curves, own, other)])
        rows = pl.ds(pl.multiple_of(low, 8), 8)
        for order in range(5):
            weights[chunk][order, 0, rows, :] = halves[0][order] + halves[1][order]
            weights[chunk][order, 1, rows, :] = halves[0][order] - halves[1][order]

    for chunk in CHUNKS:
        lax.fori_loop(
            0, COLS[chunk] // 8, lambda tile, _, chunk=chunk: (tile_step(chunk, tile), 0)[1], 0
        )
        first = (first0, first1)[chunk]
        rows = COLS[chunk]
        sign = 1.0 - 2.0 * (lax.broadcasted_iota(jnp.int32, (rows, 128), 0) % 2).astype(jnp.float32)
        for k in range(PARTS):
            source = rank ^ k
            step = jnp.full((8, 128), source, jnp.int32).astype(jnp.float32) * (math.pi / 4)
            step_re = sign * jnp.cos(step)[:1]
            step_im = sign * jnp.sin(step)[:1]
            re, im = first[source, 0], first[source, 1]
            for block in range(GRID // 128):
                lanes = slice(128 * block, 128 * (block + 1))
                for part, value in ((0, re), (1, -im)):
                    hi, lo = split(value)
                    at = slice((2 * k + part) * rows, (2 * k + part + 1) * rows)
                    final_hi[chunk][at, lanes] = hi
                    final_lo[chunk][at, lanes] = lo
                re, im = re * step_re - im * step_im, re * step_im + im * step_re
    for copy in copies:
        copy.wait()


def middle_kernel(chunk, place, got0, got1, got2, got3, weights, y_hi, y_lo, odd, *outs):
    rank = place[0]
    blocks = (got0, got1, got2, got3)
    rows, ext = COLS[chunk], EXT[chunk]
    if chunk == 1:
        first_row = lax.broadcasted_iota(jnp.int32, (MAIN, PIX), 0) == 0
        lone = jnp.logical_and(first_row, jnp.full((MAIN, PIX), rank, jnp.int32) == 0)
        top = lax.broadcasted_iota(jnp.int32, (8, PIX), 0) == 0

    def plane(index):
        whole = jnp.concatenate([b[index] for b in blocks], axis=1)
        cosines, sines = whole[:MAIN], whole[MAIN:]
        if chunk == 0:
            return cosines, sines, None
        return cosines, jnp.where(lone, 0.0, sines), jnp.where(top, sines[:8], 0.0)

    real_rows = []
    imag_rows = []

    def add_row(re, im, extra_re, extra_im):
        real_rows.append(re)
        imag_rows.append(im)
        if chunk == 1:
            real_rows.append(extra_re)
            imag_rows.append(extra_im() if callable(extra_im) else extra_im)

    cos_r, sin_r, extra_r = plane(0)
    add_row(cos_r, -sin_r, extra_r, lambda: jnp.zeros_like(extra_r))
    for m in range(2):
        cos_r, sin_r, extra_r = plane(1 + 2 * m)
        cos_i, sin_i, extra_i = plane(2 + 2 * m)
        add_row(cos_r + sin_i, cos_i - sin_r, extra_r, extra_i)
        add_row(cos_r - sin_i, -cos_i - sin_r, extra_r, lambda: -extra_i)
    data = split(jnp.concatenate(real_rows + imag_rows, axis=0))

    def y_matrix(ref):
        return jnp.concatenate(
            [jnp.concatenate([ref[rank ^ k, 0], ref[rank ^ k, 1]], axis=1) for k in range(PARTS)],
            axis=0,
        )

    turned = dot3(data, (y_matrix(y_hi), y_matrix(y_lo)), (1, 0))
    half = 5 * ext
    spec_re = turned[:half, :PIX] + turned[half:, PIX:]
    spec_im = turned[half:, :PIX] - turned[:half, PIX:]
    sums = None
    for order in range(5):

        def both(spec):
            main = spec[order * ext : order * ext + MAIN]
            if chunk == 0:
                return jnp.concatenate([main, main], axis=0)
            extra = spec[order * ext + MAIN : (order + 1) * ext]
            return jnp.concatenate([main, jnp.where(top, extra, main[16:24]), main[24:]], axis=0)

        re, im = both(spec_re), both(spec_im)
        plus, minus = weights[order, 0], weights[order, 1]
        terms = (plus * re, plus * im, minus * re, minus * im)
        sums = terms if order == 0 else tuple(a + b for a, b in zip(sums, terms))
    even_re, even_im, odd_re, odd_im = sums
    odd_cos, odd_sin = odd[0:1], odd[1:2]
    odd_re, odd_im = odd_re * odd_cos - odd_im * odd_sin, odd_re * odd_sin + odd_im * odd_cos
    filtered = split(jnp.concatenate([even_re, even_im, odd_re, odd_im], axis=0))

    def u_matrix(ref):
        return jnp.concatenate(
            [jnp.concatenate([ref[rank ^ k, 0], ref[rank ^ k, 1]], axis=0) for k in range(PARTS)],
            axis=0,
        )

    back = dot3(filtered, (u_matrix(y_hi), u_matrix(y_lo)), (1, 1))
    for k in range(PARTS):
        cos_part = back[:, 2 * ROWS * k : 2 * ROWS * k + ROWS]
        sin_part = back[:, 2 * ROWS * k + ROWS : 2 * ROWS * (k + 1)]
        for parity in range(2):
            base = 2 * rows * parity
            re, im = slice(base, base + rows), slice(base + rows, base + 2 * rows)
            lanes = slice(parity * ROWS, (parity + 1) * ROWS)
            outs[k][0:rows, lanes] = cos_part[re] - sin_part[im]
            outs[k][rows : 2 * rows, lanes] = sin_part[re] + cos_part[im]


def gathered(blocks):
    return split(jnp.concatenate([b[...] for b in blocks], axis=0))


def part_kernel(got0, got1, got2, got3, final_hi, final_lo, part):
    data = gathered((got0, got1, got2, got3))
    part[...] = dot3(data, (final_hi[...], final_lo[...]), (0, 0))


def final_kernel(got0, got1, got2, got3, final_hi, final_lo, part, out, woven, sems):
    data = gathered((got0, got1, got2, got3))
    copies = []
    for strip in range(GRID // 256):
        lanes = slice(256 * strip, 256 * (strip + 1))
        picture = part[:, lanes] + dot3(data, (final_hi[:, lanes], final_lo[:, lanes]), (0, 0))
        for block in range(2):
            at = 2 * strip + block
            piece = slice(128 * block, 128 * (block + 1))
            woven[at, pl.ds(0, ROWS, 2), :] = picture[:ROWS, piece]
            woven[at, pl.ds(1, ROWS, 2), :] = picture[ROWS:, piece]
            copy = pltpu.make_async_copy(
                woven.at[at], out.at[:, pl.ds(128 * at, 128)], sems.at[at]
            )
            copy.start()
            copies.append(copy)
    for copy in copies:
        copy.wait()


def smem():
    return pl.BlockSpec(memory_space=pltpu.SMEM)


def vmem():
    return pl.BlockSpec(memory_space=pltpu.VMEM)


def hbm():
    return pl.BlockSpec(memory_space=pltpu.HBM)


def f32(*shape):
    return jax.ShapeDtypeStruct(shape, jnp.float32)


def bf16(*shape):
    return jax.ShapeDtypeStruct(shape, jnp.bfloat16)


def call(kernel, out_shape, in_specs, out_specs=None, scratch=(), limit=24):
    if out_specs is None:
        out_specs = jax.tree.map(lambda _: vmem(), out_shape)
    return pl.pallas_call(
        kernel,
        out_shape=out_shape,
        in_specs=in_specs,
        out_specs=out_specs,
        scratch_shapes=list(scratch),
        compiler_params=pltpu.CompilerParams(vmem_limit_bytes=limit * 1024 * 1024),
    )


def from_partners(blocks):
    got = [blocks[0]]
    for k in range(1, PARTS):
        got.append(lax.ppermute(blocks[k], "row", [(i, i ^ k) for i in range(PARTS)]))
    return got


def per_device(frames, phase_offset, order_gain, band_shift):
    (x_hi, x_lo), (y_hi, y_lo), first, odd = tables()
    rank = lax.axis_index("row")
    place = rank.reshape(1).astype(jnp.int32)
    two = pltpu.SemaphoreType.DMA((2,))

    sums, frames = call(
        sums_kernel,
        [f32(8, 128), bf16(PHASES, ROWS, PIX)],
        [hbm()],
        scratch=[pltpu.SemaphoreType.DMA((PHASES,))],
    )(frames)
    sums = from_partners([sums] * PARTS)
    turns, phases, x_hi, x_lo = call(
        phase_kernel,
        [f32(4, ROWS, PIX), f32(4, 8, 128)] + [bf16(*x_hi.shape)] * 2,
        [smem()] * 3 + [hbm()] * 2,
        scratch=[two],
    )(place, band_shift, phase_offset, x_hi, x_lo)
    block = f32(5, 2 * MAIN, ROWS)
    *sent, band_hi, band_lo = call(
        forward_kernel,
        [block] * PARTS + [bf16(5 * ROWS, PIX)] * 2,
        [smem()] + [vmem()] * 9,
    )(place, *sums, turns, phases, frames, x_hi, x_lo)
    spectra = [from_partners(sent)]
    *sent, token = call(
        forward_rest_kernel, [block] * PARTS + [f32(8, 128)], [smem()] + [vmem()] * 4
    )(place, band_hi, band_lo, x_hi, x_lo)
    spectra.append(from_partners(sent))
    made = call(
        weights_kernel,
        [f32(5, 2, COLS[c], PIX) for c in CHUNKS]
        + [bf16(8 * COLS[c], GRID) for c in CHUNKS] * 2
        + [bf16(*y_hi.shape)] * 2,
        [smem()] * 3 + [vmem()] * 3 + [hbm()] * 2,
        scratch=[two],
    )(place, order_gain, band_shift, token, *first, y_hi, y_lo)
    weights, final_hi, final_lo, (y_hi, y_lo) = made[:2], made[2:4], made[4:6], made[6:]
    got = []
    for c in CHUNKS:
        sent = call(
            functools.partial(middle_kernel, c),
            [f32(2 * COLS[c], 2 * ROWS)] * PARTS,
            [smem()] + [vmem()] * 8,
        )(place, *spectra[c], weights[c], y_hi, y_lo, odd)
        got.append(from_partners(sent))
    part = call(part_kernel, f32(2 * ROWS, GRID), [vmem()] * 6)(*got[0], final_hi[0], final_lo[0])
    return call(
        final_kernel,
        f32(2 * ROWS, GRID),
        [vmem()] * 7,
        hbm(),
        [
            pltpu.VMEM((GRID // 128, 2 * ROWS, 128), jnp.float32),
            pltpu.SemaphoreType.DMA((GRID // 128,)),
        ],
    )(*got[1], final_hi[1], final_lo[1], part)


def solution(mesh):
    in_specs = (P("fov", None, "row", None), P("fov"), P("fov", None), P("fov", None))
    out_specs = P(("fov", "row"), None)
    return jax.shard_map(
        per_device, mesh=mesh, in_specs=in_specs, out_specs=out_specs, check_vma=False
    )
```

```python
import functools
import math

import jax
import jax.numpy as jnp
import numpy as np
from jax import lax
from jax.experimental import pallas as pl
from jax.experimental.pallas import tpu as pltpu
from jax.sharding import PartitionSpec as P


wiener = 0.1
gain_out = 8.0
cut_share = 0.45
PIX = 512
GRID = 1024
PHASES = 5
PARTS = 4
ROWS = PIX // PARTS
CHUNKS = (0, 1)
LOW = (24, 0)
MAIN = (40, 24)
FOLD_LOW = (24, 16)
FOLD = (40, 8)
COLS = (80, 32)
EXT = (40, 32)
ORDERS = (0, 1, -1, 2, -2)
ARC = (
    1.5707963050,
    -0.2145988016,
    0.0889789874,
    -0.0501743046,
    0.0308918810,
    -0.0170881256,
    0.0066700901,
    -0.0012624911,
)


def split_np(array):
    hi = array.astype(jnp.bfloat16)
    lo = (array - hi.astype(np.float32)).astype(jnp.bfloat16)
    return hi, lo


def split(array):
    hi = array.astype(jnp.bfloat16)
    lo = (array - hi.astype(jnp.float32)).astype(jnp.bfloat16)
    return hi, lo


def column_freq_np(d, chunk):
    def column(low, count):
        l = np.arange(low, low + count)
        return 64 * (l // 16) + 16 * d + l % 16

    fold = column(FOLD_LOW[chunk], FOLD[chunk]) - PIX
    if d == 0 and chunk == 1:
        fold[0] = -PIX // 2
    return np.concatenate([column(LOW[chunk], MAIN[chunk]), fold])


@functools.cache
def tables():
    index = np.arange(PIX)
    angle = 2.0 * np.pi * (np.outer(index[:ROWS], index) % PIX) / PIX
    base = np.stack([np.cos(angle), np.sin(angle)]).astype(np.float32)
    first = np.zeros((PARTS, 2, sum(COLS), 128), np.float32)
    for s in range(PARTS):
        freq = np.concatenate([column_freq_np(s, c) for c in CHUNKS])
        scale = gain_out / (GRID * GRID) * np.where(freq == 0, 1.0, 2.0)
        turn = 2.0 * np.pi * ((freq[:, None] * np.arange(128)[None, :]) % GRID) / GRID
        first[s, 0] = scale[:, None] * np.cos(turn)
        first[s, 1] = scale[:, None] * np.sin(turn)
    turn = 2.0 * np.pi * index / GRID
    odd = np.stack([np.cos(turn), np.sin(turn)]).astype(np.float32)
    return np.stack(split_np(base)), first, odd


def dot3(left, right, dims):
    lhs = jnp.concatenate([left[0], left[0], left[1]], axis=dims[0])
    rhs = jnp.concatenate([right[0], right[1], right[0]], axis=dims[1])
    return lax.dot_general(
        lhs, rhs, (((dims[0],), (dims[1],)), ((), ())), preferred_element_type=jnp.float32
    )


def turn_pair(steps):
    angle = (2.0 * math.pi / PIX) * ((steps + 256) % 512 - 256).astype(jnp.float32)
    return jnp.cos(angle), jnp.sin(angle)


def phase_kernel(place, shift, offset, source, base, frames, turns, phases, *rest):
    y_out, x_out, sem = rest[0:2], (rest[2:4], rest[4:6]), rest[6]
    copy = pltpu.make_async_copy(source.at[0], frames, sem)
    copy.start()
    rank = place[0]
    shift_y = shift[0]
    shift_x = shift[1]
    x_cos, x_sin = turn_pair(lax.broadcasted_iota(jnp.int32, (8, PIX), 1) * shift_x)
    row_at = lax.broadcasted_iota(jnp.int32, (ROWS, 128), 0) + rank * ROWS
    y_cos, y_sin = turn_pair(row_at * shift_y)
    x_cos, x_sin = x_cos[:1], x_sin[:1]
    y_cos = jnp.concatenate([y_cos] * 4, axis=1)
    y_sin = jnp.concatenate([y_sin] * 4, axis=1)
    turn_re = x_cos * y_cos - x_sin * y_sin
    turn_im = x_cos * y_sin + x_sin * y_cos
    turns[0] = turn_re
    turns[1] = turn_im
    turns[2] = turn_re * turn_re - turn_im * turn_im
    turns[3] = 2.0 * turn_re * turn_im
    phase_at = lax.broadcasted_iota(jnp.int32, (8, 128), 0).astype(jnp.float32)
    phase_at = (2.0 * math.pi / PHASES) * phase_at + offset[0]
    phases[0] = jnp.cos(phase_at)
    phases[1] = jnp.sin(phase_at)
    phases[2] = jnp.cos(2.0 * phase_at)
    phases[3] = jnp.sin(2.0 * phase_at)
    lane = lax.broadcasted_iota(jnp.int32, (1, PIX), 1)
    parity = lane % 2
    sign = (1 - lane % 4 + parity).astype(jnp.float32)
    quarter_re = jnp.where(parity == 0, sign, 0.0)
    quarter_im = jnp.where(parity == 1, sign, 0.0)
    half_turn = 1.0 - 2.0 * parity.astype(jnp.float32)
    for part in range(2):
        cosine, sine = base[part, 0].astype(jnp.float32), base[part, 1].astype(jnp.float32)
        cos_re, cos_im = cosine * quarter_re, cosine * quarter_im
        sin_re, sin_im = sine * quarter_re, sine * quarter_im
        blocks = [
            (cosine, sine),
            (cos_re - sin_im, sin_re + cos_im),
            (cosine * half_turn, sine * half_turn),
            (cos_re + sin_im, sin_re - cos_im),
        ]
        for s in range(PARTS):
            for kind in range(2):
                y_out[part][s, kind] = blocks[s][kind].astype(jnp.bfloat16)
        lone = half_turn if part == 0 else jnp.zeros_like(half_turn)
        top = lax.broadcasted_iota(jnp.int32, (8, PIX), 0) == 0
        for chunk in CHUNKS:
            for d in range(PARTS):
                pieces = []
                for kind in range(2):
                    for l in range(LOW[chunk], LOW[chunk] + MAIN[chunk], 8):
                        column = 64 * (l // 16) + 16 * d + l % 16
                        s, t = column // ROWS, column % ROWS
                        piece = blocks[s][kind][t : t + 8]
                        if column == 0 and kind == 1:
                            piece = jnp.where(top, lone, piece)
                        pieces.append(piece)
                x_out[chunk][part][d] = jnp.concatenate(pieces, axis=0).astype(jnp.bfloat16)
    copy.wait()


def spectra_rows(rank, rows, band, x_hi, x_lo, outs):
    table = (
        jnp.concatenate([x_hi[rank ^ k] for k in range(PARTS)], axis=0),
        jnp.concatenate([x_lo[rank ^ k] for k in range(PARTS)], axis=0),
    )
    spectra = dot3(table, band, (1, 1))
    for k in range(PARTS):
        for plane in range(5):
            outs[k][plane] = spectra[
                k * rows : (k + 1) * rows, plane * ROWS : (plane + 1) * ROWS
            ]


def forward_kernel(place, sums0, sums1, sums2, sums3, turns, phases, frames, x_hi, x_lo, *rest):
    outs, (band_hi, band_lo) = rest[:PARTS], rest[PARTS:]
    total = (sums0[...] + sums1[...]) + (sums2[...] + sums3[...])
    weight_all = (PIX * PIX / PHASES) / total
    acc = None
    for p in range(PHASES):
        weight = weight_all[:, p : p + 1]
        plane = frames[p].astype(jnp.float32)
        terms = [plane * weight] + [
            plane * (weight * phases[i, p : p + 1, 0:1]) for i in range(4)
        ]
        acc = terms if p == 0 else [a + b for a, b in zip(acc, terms)]
    zero, one_re, one_im, two_re, two_im = acc
    planes = [
        zero,
        one_re * turns[0] + one_im * turns[1],
        one_re * turns[1] - one_im * turns[0],
        two_re * turns[2] + two_im * turns[3],
        two_re * turns[3] - two_im * turns[2],
    ]
    for index, plane in enumerate(planes):
        hi, lo = split(plane)
        band_hi[index * ROWS : (index + 1) * ROWS, :] = hi
        band_lo[index * ROWS : (index + 1) * ROWS, :] = lo
    spectra_rows(place[0], 2 * MAIN[0], (band_hi[...], band_lo[...]), x_hi, x_lo, outs)


def forward_rest_kernel(place, band_hi, band_lo, x_hi, x_lo, *outs):
    spectra_rows(place[0], 2 * MAIN[1], (band_hi[...], band_lo[...]), x_hi, x_lo, outs)


def transfer_curve(squared):
    radius = jnp.minimum(jnp.sqrt(squared * (1.0 / (cut_share * PIX) ** 2)), 1.0)
    arc = jnp.full_like(radius, ARC[7])
    for coefficient in ARC[6::-1]:
        arc = arc * radius + coefficient
    return (2.0 / math.pi) * jnp.sqrt(1.0 - radius) * (arc - radius * jnp.sqrt(1.0 + radius))


def weights_kernel(place, gains, shift, after, weights0, weights1, y_square, y_low):
    weights = (weights0, weights1)
    rank = place[0]
    shift_y, shift_x = shift[0], shift[1]
    own = [gains[m + 2] for m in ORDERS]
    other = [gains[2 - m] for m in ORDERS]
    sub = lax.broadcasted_iota(jnp.int32, (8, 1), 0)
    lane = lax.broadcasted_iota(jnp.int32, (8, PIX), 1)
    for order, m in enumerate(ORDERS):
        y = ((lane - m * shift_y + PIX // 2) & (PIX - 1)) - PIX // 2
        y_low[order] = jnp.where(y + m * shift_y >= 0, 1.0, 0.0)
        y = y.astype(jnp.float32)
        y_square[order] = y * y

    def tile_step(chunk, tile):
        low = 8 * tile
        folded = low >= MAIN[chunk]
        l = jnp.where(folded, low - MAIN[chunk] + FOLD_LOW[chunk], low + LOW[chunk])
        freq = 64 * (l // 16) + 16 * rank + l % 16
        freq_x = jnp.where(folded, freq - PIX, freq) + sub
        if chunk == 1:
            lone = jnp.logical_and(low == MAIN[1], rank == 0).astype(jnp.int32)
            freq_x = jnp.where(jnp.where(sub == 0, lone, 0) == 1, -PIX // 2, freq_x)
        dens = [jnp.full((8, PIX), wiener, jnp.float32)] * 4
        curves = []
        for order, m in enumerate(ORDERS):
            x = (freq_x - m * shift_x).astype(jnp.float32)
            curve = transfer_curve(x * x + y_square[order])
            power = curve * curve
            power_low = power * y_low[order]
            power_high = power - power_low
            g, h = own[order] * own[order], other[order] * other[order]
            dens = [
                dens[0] + g * power_low,
                dens[1] + g * power_high,
                dens[2] + h * power_low,
                dens[3] + h * power_high,
            ]
            curves.append(curve)
        own_low, own_high, other_low, other_high = [0.5 / den for den in dens]
        rows = pl.ds(pl.multiple_of(low, 8), 8)
        for order in range(5):
            is_low = y_low[order] > 0.5
            own_den = jnp.where(is_low, own_low, own_high)
            other_den = jnp.where(is_low, other_low, other_high)
            weight = curves[order] * (own[order] * own_den + other[order] * other_den)
            weights[chunk][order, 0, rows, :] = weight
            weights[chunk][order, 1, rows, :] = jnp.where(is_low, weight, -weight)

    for chunk in CHUNKS:
        lax.fori_loop(
            0, COLS[chunk] // 8, lambda tile, _, chunk=chunk: (tile_step(chunk, tile), 0)[1], 0
        )


def table_kernel(place, first, after, hi0, hi1, lo0, lo1):
    outs = ((hi0, lo0), (hi1, lo1))
    rank = place[0]
    turn = lax.broadcasted_iota(jnp.int32, (8, 128), 0).astype(jnp.float32) * (math.pi / 4)
    turn_re, turn_im = jnp.cos(turn), jnp.sin(turn)
    low = 0
    for chunk in CHUNKS:
        rows = COLS[chunk]
        step_re = jnp.concatenate([turn_re] * (rows // 8), axis=0)
        step_im = jnp.concatenate([turn_im] * (rows // 8), axis=0)
        for k in range(PARTS):
            source = rank ^ k
            re, im = first[source, 0, low : low + rows], first[source, 1, low : low + rows]
            for block in range(GRID // 128):
                lanes = slice(128 * block, 128 * (block + 1))
                for part, value in ((0, re), (1, -im)):
                    at = slice((2 * k + part) * rows, (2 * k + part + 1) * rows)
                    outs[chunk][0][at, lanes], outs[chunk][1][at, lanes] = split(value)
                re, im = re * step_re - im * step_im, re * step_im + im * step_re
        low += rows


def middle_kernel(chunk, place, got0, got1, got2, got3, weights, y_hi, y_lo, odd, *outs):
    rank = place[0]
    blocks = (got0, got1, got2, got3)
    rows, ext, count = COLS[chunk], EXT[chunk], MAIN[chunk]
    if chunk == 1:
        first_row = lax.broadcasted_iota(jnp.int32, (count, PIX), 0) == 0
        lone = jnp.logical_and(first_row, jnp.full((count, PIX), rank, jnp.int32) == 0)
        top = lax.broadcasted_iota(jnp.int32, (8, PIX), 0) == 0
        swap = lone[:8]

    def plane(index):
        whole = jnp.concatenate([b[index] for b in blocks], axis=1)
        cosines, sines = whole[:count], whole[count:]
        if chunk == 0:
            return cosines, sines, None
        return cosines, jnp.where(lone, 0.0, sines), jnp.where(top, sines[:8], 0.0)

    real_rows = []
    imag_rows = []

    def add_row(re, im, extra_re, extra_im):
        real_rows.append(re)
        imag_rows.append(im)
        if chunk == 1:
            real_rows.append(extra_re)
            imag_rows.append(extra_im() if callable(extra_im) else extra_im)

    cos_r, sin_r, extra_r = plane(0)
    add_row(cos_r, -sin_r, extra_r, lambda: jnp.zeros_like(extra_r))
    for m in range(2):
        cos_r, sin_r, extra_r = plane(1 + 2 * m)
        cos_i, sin_i, extra_i = plane(2 + 2 * m)
        add_row(cos_r + sin_i, cos_i - sin_r, extra_r, extra_i)
        add_row(cos_r - sin_i, -cos_i - sin_r, extra_r, lambda: -extra_i)
    data = split(jnp.concatenate(real_rows + imag_rows, axis=0))

    def y_matrix(ref):
        return jnp.concatenate(
            [jnp.concatenate([ref[rank ^ k, 0], ref[rank ^ k, 1]], axis=1) for k in range(PARTS)],
            axis=0,
        )

    turned = dot3(data, (y_matrix(y_hi), y_matrix(y_lo)), (1, 0))
    half = 5 * ext
    spec_re = turned[:half, :PIX] + turned[half:, PIX:]
    spec_im = turned[half:, :PIX] - turned[:half, PIX:]
    sums = None
    for order in range(5):

        def both(spec):
            main = spec[order * ext : order * ext + count]
            if chunk == 0:
                return jnp.concatenate([main, main], axis=0)
            extra = spec[order * ext + count : (order + 1) * ext]
            return jnp.concatenate(
                [main, jnp.where(swap, extra, main[16:24])] + ([main[24:]] if count > 24 else []), axis=0
            )

        re, im = both(spec_re), both(spec_im)
        plus, minus = weights[order, 0], weights[order, 1]
        terms = (plus * re, plus * im, minus * re, minus * im)
        sums = terms if order == 0 else tuple(a + b for a, b in zip(sums, terms))
    even_re, even_im, odd_re, odd_im = sums
    odd_cos, odd_sin = odd[0:1], odd[1:2]
    odd_re, odd_im = odd_re * odd_cos - odd_im * odd_sin, odd_re * odd_sin + odd_im * odd_cos
    filtered = split(jnp.concatenate([even_re, even_im, odd_re, odd_im], axis=0))

    def u_matrix(ref):
        return jnp.concatenate(
            [jnp.concatenate([ref[rank ^ k, 0], ref[rank ^ k, 1]], axis=0) for k in range(PARTS)],
            axis=0,
        )

    back = dot3(filtered, (u_matrix(y_hi), u_matrix(y_lo)), (1, 1))
    for k in range(PARTS):
        cos_part = back[:, 2 * ROWS * k : 2 * ROWS * k + ROWS]
        sin_part = back[:, 2 * ROWS * k + ROWS : 2 * ROWS * (k + 1)]
        for parity in range(2):
            base = 2 * rows * parity
            re, im = slice(base, base + rows), slice(base + rows, base + 2 * rows)
            lanes = slice(parity * ROWS, (parity + 1) * ROWS)
            outs[k][0:rows, lanes] = cos_part[re] - sin_part[im]
            outs[k][rows : 2 * rows, lanes] = sin_part[re] + cos_part[im]


def gathered(blocks):
    return split(jnp.concatenate([b[...] for b in blocks], axis=0))


def part_kernel(got0, got1, got2, got3, final_hi, final_lo, part):
    data = gathered((got0, got1, got2, got3))
    part[...] = dot3(data, (final_hi[...], final_lo[...]), (0, 0))


def final_kernel(got0, got1, got2, got3, final_hi, final_lo, part, out, woven, sems):
    data = gathered((got0, got1, got2, got3))
    copies = []
    for strip in range(GRID // 256):
        lanes = slice(256 * strip, 256 * (strip + 1))
        picture = part[:, lanes] + dot3(data, (final_hi[:, lanes], final_lo[:, lanes]), (0, 0))
        for block in range(2):
            at = 2 * strip + block
            piece = slice(128 * block, 128 * (block + 1))
            woven[at, pl.ds(0, ROWS, 2), :] = picture[:ROWS, piece]
            woven[at, pl.ds(1, ROWS, 2), :] = picture[ROWS:, piece]
            copy = pltpu.make_async_copy(
                woven.at[at], out.at[:, pl.ds(128 * at, 128)], sems.at[at]
            )
            copy.start()
            copies.append(copy)
    for copy in copies:
        copy.wait()


def smem():
    return pl.BlockSpec(memory_space=pltpu.SMEM)


def vmem():
    return pl.BlockSpec(memory_space=pltpu.VMEM)


def hbm():
    return pl.BlockSpec(memory_space=pltpu.HBM)


def f32(*shape):
    return jax.ShapeDtypeStruct(shape, jnp.float32)


def bf16(*shape):
    return jax.ShapeDtypeStruct(shape, jnp.bfloat16)


def call(kernel, out_shape, in_specs, out_specs=None, scratch=(), limit=24):
    if out_specs is None:
        out_specs = jax.tree.map(lambda _: vmem(), out_shape)
    return pl.pallas_call(
        kernel,
        out_shape=out_shape,
        in_specs=in_specs,
        out_specs=out_specs,
        scratch_shapes=list(scratch),
        compiler_params=pltpu.CompilerParams(vmem_limit_bytes=limit * 1024 * 1024),
    )


def from_partners(blocks):
    got = [blocks[0]]
    for k in range(1, PARTS):
        got.append(lax.ppermute(blocks[k], "row", [(i, i ^ k) for i in range(PARTS)]))
    return got


def reconstruct(frames, phase_offset, order_gain, band_shift):
    base, first, odd = tables()
    order_gain, band_shift = order_gain[0], band_shift[0]
    rank = lax.axis_index("row")
    place = rank.reshape(1).astype(jnp.int32)

    sums = jnp.sum(frames.astype(jnp.float32), axis=(2, 3))
    sums = from_partners([sums] * PARTS)
    frames, turns, phases, y_hi, y_lo, *x_parts = call(
        phase_kernel,
        [bf16(PHASES, ROWS, PIX), f32(4, ROWS, PIX), f32(4, 8, 128)]
        + [bf16(PARTS, 2, ROWS, PIX)] * 2
        + [bf16(PARTS, 2 * MAIN[c], PIX) for c in CHUNKS for _ in range(2)],
        [smem()] * 3 + [hbm(), vmem()],
        scratch=[pltpu.SemaphoreType.DMA],
    )(place, band_shift, phase_offset, frames, base)
    blocks = [f32(5, 2 * MAIN[c], ROWS) for c in CHUNKS]
    *sent, band_hi, band_lo = call(
        forward_kernel,
        [blocks[0]] * PARTS + [bf16(5 * ROWS, PIX)] * 2,
        [smem()] + [vmem()] * 9,
    )(place, *sums, turns, phases, frames, *x_parts[:2])
    spectra = [from_partners(sent)]
    sent = call(forward_rest_kernel, [blocks[1]] * PARTS, [smem()] + [vmem()] * 4)(
        place, band_hi, band_lo, *x_parts[2:]
    )
    spectra.append(from_partners(sent))
    weights = call(
        weights_kernel,
        [f32(5, 2, COLS[c], PIX) for c in CHUNKS],
        [smem()] * 3 + [vmem()],
        scratch=[pltpu.VMEM((5, 8, PIX), jnp.float32)] * 2,
    )(place, order_gain, band_shift, sent[0])
    hi0, hi1, lo0, lo1 = call(
        table_kernel,
        [bf16(8 * COLS[c], GRID) for c in CHUNKS] * 2,
        [smem()] + [vmem()] * 2,
    )(place, first, sent[0])
    got = []
    for c in CHUNKS:
        sent = call(
            functools.partial(middle_kernel, c),
            [f32(2 * COLS[c], 2 * ROWS)] * PARTS,
            [smem()] + [vmem()] * 8,
        )(place, *spectra[c], weights[c], y_hi, y_lo, odd)
        got.append(from_partners(sent))
    part = call(part_kernel, f32(2 * ROWS, GRID), [vmem()] * 6)(*got[0], hi0, lo0)
    return call(
        final_kernel,
        f32(2 * ROWS, GRID),
        [vmem()] * 7,
        hbm(),
        [
            pltpu.VMEM((GRID // 128, 2 * ROWS, 128), jnp.float32),
            pltpu.SemaphoreType.DMA((GRID // 128,)),
        ],
    )(*got[1], hi1, lo1, part)


def solution(mesh):
    in_specs = (P("fov", None, "row", None), P("fov"), P("fov", None), P("fov", None))
    out_specs = P(("fov", "row"), None)
    return jax.shard_map(
        reconstruct, mesh=mesh, in_specs=in_specs, out_specs=out_specs, check_vma=False
    )
```

```python
import functools
import math

import jax
import jax.numpy as jnp
import numpy as np
from jax import lax
from jax.experimental import pallas as pl
from jax.experimental.pallas import tpu as pltpu
from jax.sharding import PartitionSpec as P


wiener = 0.1
gain_out = 8.0
cut_share = 0.45
PIX = 512
GRID = 1024
PHASES = 5
PARTS = 4
ROWS = PIX // PARTS
CHUNKS = (0, 1)
LOW = (24, 0)
MAIN = (40, 24)
FOLD_LOW = (24, 16)
FOLD = (40, 8)
COLS = (80, 32)
EXT = (40, 32)
ORDERS = (0, 1, -1, 2, -2)
ARC = (
    1.5707963050,
    -0.2145988016,
    0.0889789874,
    -0.0501743046,
    0.0308918810,
    -0.0170881256,
    0.0066700901,
    -0.0012624911,
)


def split_np(array):
    hi = array.astype(jnp.bfloat16)
    lo = (array - hi.astype(np.float32)).astype(jnp.bfloat16)
    return hi, lo


def split(array):
    hi = array.astype(jnp.bfloat16)
    lo = (array - hi.astype(jnp.float32)).astype(jnp.bfloat16)
    return hi, lo


def column_freq_np(d, chunk):
    def column(low, count):
        l = np.arange(low, low + count)
        return 64 * (l // 16) + 16 * d + l % 16

    fold = column(FOLD_LOW[chunk], FOLD[chunk]) - PIX
    if d == 0 and chunk == 1:
        fold[0] = -PIX // 2
    return np.concatenate([column(LOW[chunk], MAIN[chunk]), fold])


@functools.cache
def tables():
    index = np.arange(PIX)
    angle = 2.0 * np.pi * (np.outer(index[:ROWS], index) % PIX) / PIX
    base = np.stack([np.cos(angle), np.sin(angle)]).astype(np.float32)
    first = np.zeros((PARTS, 2, sum(COLS), 128), np.float32)
    for s in range(PARTS):
        freq = np.concatenate([column_freq_np(s, c) for c in CHUNKS])
        scale = gain_out / (GRID * GRID) * np.where(freq == 0, 1.0, 2.0)
        turn = 2.0 * np.pi * ((freq[:, None] * np.arange(128)[None, :]) % GRID) / GRID
        first[s, 0] = scale[:, None] * np.cos(turn)
        first[s, 1] = scale[:, None] * np.sin(turn)
    turn = 2.0 * np.pi * index / GRID
    odd = np.stack([np.cos(turn), np.sin(turn)]).astype(np.float32)
    return np.stack(split_np(base)), first, odd


def dot3(left, right, dims):
    lhs = jnp.concatenate([left[0], left[0], left[1]], axis=dims[0])
    rhs = jnp.concatenate([right[0], right[1], right[0]], axis=dims[1])
    return lax.dot_general(
        lhs, rhs, (((dims[0],), (dims[1],)), ((), ())), preferred_element_type=jnp.float32
    )


def turn_pair(steps):
    angle = (2.0 * math.pi / PIX) * ((steps + 256) % 512 - 256).astype(jnp.float32)
    return jnp.cos(angle), jnp.sin(angle)


def phase_kernel(place, shift, offset, source, base_far, frames, turns, phases, *rest):
    y_out, x_out, base, sems = rest[0:2], (rest[2:4], rest[4:6]), rest[6], rest[7]
    base_copy = pltpu.make_async_copy(base_far, base, sems.at[0])
    base_copy.start()
    copy = pltpu.make_async_copy(source.at[0], frames, sems.at[1])
    copy.start()
    rank = place[0]
    shift_y = shift[0]
    shift_x = shift[1]
    x_cos, x_sin = turn_pair(lax.broadcasted_iota(jnp.int32, (8, PIX), 1) * shift_x)
    row_at = lax.broadcasted_iota(jnp.int32, (ROWS, 128), 0) + rank * ROWS
    y_cos, y_sin = turn_pair(row_at * shift_y)
    x_cos, x_sin = x_cos[:1], x_sin[:1]
    y_cos = jnp.concatenate([y_cos] * 4, axis=1)
    y_sin = jnp.concatenate([y_sin] * 4, axis=1)
    turn_re = x_cos * y_cos - x_sin * y_sin
    turn_im = x_cos * y_sin + x_sin * y_cos
    turns[0] = turn_re
    turns[1] = turn_im
    turns[2] = turn_re * turn_re - turn_im * turn_im
    turns[3] = 2.0 * turn_re * turn_im
    phase_at = lax.broadcasted_iota(jnp.int32, (8, 128), 0).astype(jnp.float32)
    phase_at = (2.0 * math.pi / PHASES) * phase_at + offset[0]
    phases[0] = jnp.cos(phase_at)
    phases[1] = jnp.sin(phase_at)
    phases[2] = jnp.cos(2.0 * phase_at)
    phases[3] = jnp.sin(2.0 * phase_at)
    lane = lax.broadcasted_iota(jnp.int32, (1, PIX), 1)
    parity = lane % 2
    sign = (1 - lane % 4 + parity).astype(jnp.float32)
    quarter_re = jnp.where(parity == 0, sign, 0.0)
    quarter_im = jnp.where(parity == 1, sign, 0.0)
    half_turn = 1.0 - 2.0 * parity.astype(jnp.float32)
    base_copy.wait()
    for part in range(2):
        cosine, sine = base[part, 0].astype(jnp.float32), base[part, 1].astype(jnp.float32)
        cos_re, cos_im = cosine * quarter_re, cosine * quarter_im
        sin_re, sin_im = sine * quarter_re, sine * quarter_im
        blocks = [
            (cosine, sine),
            (cos_re - sin_im, sin_re + cos_im),
            (cosine * half_turn, sine * half_turn),
            (cos_re + sin_im, sin_re - cos_im),
        ]
        for s in range(PARTS):
            for kind in range(2):
                y_out[part][s, kind] = blocks[s][kind].astype(jnp.bfloat16)
        lone = half_turn if part == 0 else jnp.zeros_like(half_turn)
        top = lax.broadcasted_iota(jnp.int32, (8, PIX), 0) == 0
        for chunk in CHUNKS:
            for d in range(PARTS):
                pieces = []
                for kind in range(2):
                    for l in range(LOW[chunk], LOW[chunk] + MAIN[chunk], 8):
                        column = 64 * (l // 16) + 16 * d + l % 16
                        s, t = column // ROWS, column % ROWS
                        piece = blocks[s][kind][t : t + 8]
                        if column == 0 and kind == 1:
                            piece = jnp.where(top, lone, piece)
                        pieces.append(piece)
                x_out[chunk][part][d] = jnp.concatenate(pieces, axis=0).astype(jnp.bfloat16)
    copy.wait()


def spectra_rows(rank, rows, band, x_hi, x_lo, outs):
    table = (
        jnp.concatenate([x_hi[rank ^ k] for k in range(PARTS)], axis=0),
        jnp.concatenate([x_lo[rank ^ k] for k in range(PARTS)], axis=0),
    )
    spectra = dot3(table, band, (1, 1))
    for k in range(PARTS):
        for plane in range(5):
            outs[k][plane] = spectra[
                k * rows : (k + 1) * rows, plane * ROWS : (plane + 1) * ROWS
            ]


def forward_kernel(place, sums0, sums1, sums2, sums3, turns, phases, frames, x_hi, x_lo, *rest):
    outs, (band_hi, band_lo) = rest[:PARTS], rest[PARTS:]
    total = (sums0[...] + sums1[...]) + (sums2[...] + sums3[...])
    weight_all = (PIX * PIX / PHASES) / total
    acc = None
    for p in range(PHASES):
        weight = weight_all[:, p : p + 1]
        plane = frames[p].astype(jnp.float32)
        terms = [plane * weight] + [
            plane * (weight * phases[i, p : p + 1, 0:1]) for i in range(4)
        ]
        acc = terms if p == 0 else [a + b for a, b in zip(acc, terms)]
    zero, one_re, one_im, two_re, two_im = acc
    planes = [
        zero,
        one_re * turns[0] + one_im * turns[1],
        one_re * turns[1] - one_im * turns[0],
        two_re * turns[2] + two_im * turns[3],
        two_re * turns[3] - two_im * turns[2],
    ]
    for index, plane in enumerate(planes):
        hi, lo = split(plane)
        band_hi[index * ROWS : (index + 1) * ROWS, :] = hi
        band_lo[index * ROWS : (index + 1) * ROWS, :] = lo
    spectra_rows(place[0], 2 * MAIN[0], (band_hi[...], band_lo[...]), x_hi, x_lo, outs)


def forward_rest_kernel(place, band_hi, band_lo, x_hi, x_lo, *outs):
    spectra_rows(place[0], 2 * MAIN[1], (band_hi[...], band_lo[...]), x_hi, x_lo, outs)


def transfer_curve(squared):
    radius = jnp.minimum(jnp.sqrt(squared * (1.0 / (cut_share * PIX) ** 2)), 1.0)
    arc = jnp.full_like(radius, ARC[7])
    for coefficient in ARC[6::-1]:
        arc = arc * radius + coefficient
    return (2.0 / math.pi) * jnp.sqrt(1.0 - radius) * (arc - radius * jnp.sqrt(1.0 + radius))


def weights_kernel(place, gains, shift, after, weights0, weights1, y_square, y_low):
    weights = (weights0, weights1)
    rank = place[0]
    shift_y, shift_x = shift[0], shift[1]
    own = [gains[m + 2] for m in ORDERS]
    other = [gains[2 - m] for m in ORDERS]
    sub = lax.broadcasted_iota(jnp.int32, (8, 1), 0)
    lane = lax.broadcasted_iota(jnp.int32, (8, PIX), 1)
    for order, m in enumerate(ORDERS):
        y = ((lane - m * shift_y + PIX // 2) & (PIX - 1)) - PIX // 2
        y_low[order] = jnp.where(y + m * shift_y >= 0, 1.0, 0.0)
        y = y.astype(jnp.float32)
        y_square[order] = y * y

    def tile_step(chunk, tile):
        low = 8 * tile
        folded = low >= MAIN[chunk]
        l = jnp.where(folded, low - MAIN[chunk] + FOLD_LOW[chunk], low + LOW[chunk])
        freq = 64 * (l // 16) + 16 * rank + l % 16
        freq_x = jnp.where(folded, freq - PIX, freq) + sub
        if chunk == 1:
            lone = jnp.logical_and(low == MAIN[1], rank == 0).astype(jnp.int32)
            freq_x = jnp.where(jnp.where(sub == 0, lone, 0) == 1, -PIX // 2, freq_x)
        dens = [jnp.full((8, PIX), wiener, jnp.float32)] * 4
        curves = []
        for order, m in enumerate(ORDERS):
            x = (freq_x - m * shift_x).astype(jnp.float32)
            curve = transfer_curve(x * x + y_square[order])
            power = curve * curve
            power_low = power * y_low[order]
            power_high = power - power_low
            g, h = own[order] * own[order], other[order] * other[order]
            dens = [
                dens[0] + g * power_low,
                dens[1] + g * power_high,
                dens[2] + h * power_low,
                dens[3] + h * power_high,
            ]
            curves.append(curve)
        own_low, own_high, other_low, other_high = [0.5 / den for den in dens]
        rows = pl.ds(pl.multiple_of(low, 8), 8)
        for order in range(5):
            is_low = y_low[order] > 0.5
            own_den = jnp.where(is_low, own_low, own_high)
            other_den = jnp.where(is_low, other_low, other_high)
            weight = curves[order] * (own[order] * own_den + other[order] * other_den)
            weights[chunk][order, 0, rows, :] = weight
            weights[chunk][order, 1, rows, :] = jnp.where(is_low, weight, -weight)

    for chunk in CHUNKS:
        lax.fori_loop(
            0, COLS[chunk] // 8, lambda tile, _, chunk=chunk: (tile_step(chunk, tile), 0)[1], 0
        )


def table_kernel(place, first, after, hi0, hi1, lo0, lo1):
    outs = ((hi0, lo0), (hi1, lo1))
    rank = place[0]
    turn = lax.broadcasted_iota(jnp.int32, (8, 128), 0).astype(jnp.float32) * (math.pi / 4)
    turn_re, turn_im = jnp.cos(turn), jnp.sin(turn)
    low = 0
    for chunk in CHUNKS:
        rows = COLS[chunk]
        step_re = jnp.concatenate([turn_re] * (rows // 8), axis=0)
        step_im = jnp.concatenate([turn_im] * (rows // 8), axis=0)
        for k in range(PARTS):
            source = rank ^ k
            re, im = first[source, 0, low : low + rows], first[source, 1, low : low + rows]
            for block in range(GRID // 128):
                lanes = slice(128 * block, 128 * (block + 1))
                for part, value in ((0, re), (1, -im)):
                    at = slice((2 * k + part) * rows, (2 * k + part + 1) * rows)
                    outs[chunk][0][at, lanes], outs[chunk][1][at, lanes] = split(value)
                re, im = re * step_re - im * step_im, re * step_im + im * step_re
        low += rows


def middle_kernel(chunk, place, got0, got1, got2, got3, weights, y_hi, y_lo, odd, *outs):
    rank = place[0]
    blocks = (got0, got1, got2, got3)
    rows, ext, count = COLS[chunk], EXT[chunk], MAIN[chunk]
    if chunk == 1:
        first_row = lax.broadcasted_iota(jnp.int32, (count, PIX), 0) == 0
        lone = jnp.logical_and(first_row, jnp.full((count, PIX), rank, jnp.int32) == 0)
        top = lax.broadcasted_iota(jnp.int32, (8, PIX), 0) == 0
        swap = lone[:8]

    def plane(index):
        whole = jnp.concatenate([b[index] for b in blocks], axis=1)
        cosines, sines = whole[:count], whole[count:]
        if chunk == 0:
            return cosines, sines, None
        return cosines, jnp.where(lone, 0.0, sines), jnp.where(top, sines[:8], 0.0)

    real_rows = []
    imag_rows = []

    def add_row(re, im, extra_re, extra_im):
        real_rows.append(re)
        imag_rows.append(im)
        if chunk == 1:
            real_rows.append(extra_re)
            imag_rows.append(extra_im() if callable(extra_im) else extra_im)

    cos_r, sin_r, extra_r = plane(0)
    add_row(cos_r, -sin_r, extra_r, lambda: jnp.zeros_like(extra_r))
    for m in range(2):
        cos_r, sin_r, extra_r = plane(1 + 2 * m)
        cos_i, sin_i, extra_i = plane(2 + 2 * m)
        add_row(cos_r + sin_i, cos_i - sin_r, extra_r, extra_i)
        add_row(cos_r - sin_i, -cos_i - sin_r, extra_r, lambda: -extra_i)
    data = split(jnp.concatenate(real_rows + imag_rows, axis=0))

    def y_matrix(ref):
        return jnp.concatenate(
            [jnp.concatenate([ref[rank ^ k, 0], ref[rank ^ k, 1]], axis=1) for k in range(PARTS)],
            axis=0,
        )

    turned = dot3(data, (y_matrix(y_hi), y_matrix(y_lo)), (1, 0))
    half = 5 * ext
    spec_re = turned[:half, :PIX] + turned[half:, PIX:]
    spec_im = turned[half:, :PIX] - turned[:half, PIX:]
    sums = None
    for order in range(5):

        def both(spec):
            main = spec[order * ext : order * ext + count]
            if chunk == 0:
                return jnp.concatenate([main, main], axis=0)
            extra = spec[order * ext + count : (order + 1) * ext]
            return jnp.concatenate(
                [main, jnp.where(swap, extra, main[16:24])] + ([main[24:]] if count > 24 else []), axis=0
            )

        re, im = both(spec_re), both(spec_im)
        plus, minus = weights[order, 0], weights[order, 1]
        terms = (plus * re, plus * im, minus * re, minus * im)
        sums = terms if order == 0 else tuple(a + b for a, b in zip(sums, terms))
    even_re, even_im, odd_re, odd_im = sums
    odd_cos, odd_sin = odd[0:1], odd[1:2]
    odd_re, odd_im = odd_re * odd_cos - odd_im * odd_sin, odd_re * odd_sin + odd_im * odd_cos
    filtered = split(jnp.concatenate([even_re, even_im, odd_re, odd_im], axis=0))

    def u_matrix(ref):
        return jnp.concatenate(
            [jnp.concatenate([ref[rank ^ k, 0], ref[rank ^ k, 1]], axis=0) for k in range(PARTS)],
            axis=0,
        )

    back = dot3(filtered, (u_matrix(y_hi), u_matrix(y_lo)), (1, 1))
    for k in range(PARTS):
        cos_part = back[:, 2 * ROWS * k : 2 * ROWS * k + ROWS]
        sin_part = back[:, 2 * ROWS * k + ROWS : 2 * ROWS * (k + 1)]
        for parity in range(2):
            base = 2 * rows * parity
            re, im = slice(base, base + rows), slice(base + rows, base + 2 * rows)
            lanes = slice(parity * ROWS, (parity + 1) * ROWS)
            outs[k][0:rows, lanes] = cos_part[re] - sin_part[im]
            outs[k][rows : 2 * rows, lanes] = sin_part[re] + cos_part[im]


def gathered(blocks):
    return split(jnp.concatenate([b[...] for b in blocks], axis=0))


def part_kernel(got0, got1, got2, got3, final_hi, final_lo, part):
    data = gathered((got0, got1, got2, got3))
    part[...] = dot3(data, (final_hi[...], final_lo[...]), (0, 0))


def final_kernel(got0, got1, got2, got3, final_hi, final_lo, part, out, woven, sems):
    data = gathered((got0, got1, got2, got3))
    copies = []
    for strip in range(GRID // 256):
        lanes = slice(256 * strip, 256 * (strip + 1))
        picture = part[:, lanes] + dot3(data, (final_hi[:, lanes], final_lo[:, lanes]), (0, 0))
        for block in range(2):
            at = 2 * strip + block
            piece = slice(128 * block, 128 * (block + 1))
            woven[at, pl.ds(0, ROWS, 2), :] = picture[:ROWS, piece]
            woven[at, pl.ds(1, ROWS, 2), :] = picture[ROWS:, piece]
            copy = pltpu.make_async_copy(
                woven.at[at], out.at[:, pl.ds(128 * at, 128)], sems.at[at]
            )
            copy.start()
            copies.append(copy)
    for copy in copies:
        copy.wait()


def smem():
    return pl.BlockSpec(memory_space=pltpu.SMEM)


def vmem():
    return pl.BlockSpec(memory_space=pltpu.VMEM)


def hbm():
    return pl.BlockSpec(memory_space=pltpu.HBM)


def f32(*shape):
    return jax.ShapeDtypeStruct(shape, jnp.float32)


def bf16(*shape):
    return jax.ShapeDtypeStruct(shape, jnp.bfloat16)


def call(kernel, out_shape, in_specs, out_specs=None, scratch=(), limit=24):
    if out_specs is None:
        out_specs = jax.tree.map(lambda _: vmem(), out_shape)
    return pl.pallas_call(
        kernel,
        out_shape=out_shape,
        in_specs=in_specs,
        out_specs=out_specs,
        scratch_shapes=list(scratch),
        compiler_params=pltpu.CompilerParams(vmem_limit_bytes=limit * 1024 * 1024),
    )


def from_partners(blocks):
    got = [blocks[0]]
    for k in range(1, PARTS):
        got.append(lax.ppermute(blocks[k], "row", [(i, i ^ k) for i in range(PARTS)]))
    return got


def reconstruct(frames, phase_offset, order_gain, band_shift):
    base, first, odd = tables()
    order_gain, band_shift = order_gain[0], band_shift[0]
    rank = lax.axis_index("row")
    place = rank.reshape(1).astype(jnp.int32)

    sums = jnp.sum(frames.astype(jnp.float32), axis=(2, 3))
    sums = from_partners([sums] * PARTS)
    frames, turns, phases, y_hi, y_lo, *x_parts = call(
        phase_kernel,
        [bf16(PHASES, ROWS, PIX), f32(4, ROWS, PIX), f32(4, 8, 128)]
        + [bf16(PARTS, 2, ROWS, PIX)] * 2
        + [bf16(PARTS, 2 * MAIN[c], PIX) for c in CHUNKS for _ in range(2)],
        [smem()] * 3 + [hbm(), hbm()],
        scratch=[pltpu.VMEM(base.shape, jnp.bfloat16), pltpu.SemaphoreType.DMA((2,))],
    )(
        place,
        band_shift,
        phase_offset,
        pltpu.with_memory_space_constraint(frames, pltpu.HBM),
        pltpu.with_memory_space_constraint(base, pltpu.HBM),
    )
    blocks = [f32(5, 2 * MAIN[c], ROWS) for c in CHUNKS]
    *sent, band_hi, band_lo = call(
        forward_kernel,
        [blocks[0]] * PARTS + [bf16(5 * ROWS, PIX)] * 2,
        [smem()] + [vmem()] * 9,
    )(place, *sums, turns, phases, frames, *x_parts[:2])
    spectra = [from_partners(sent)]
    sent = call(forward_rest_kernel, [blocks[1]] * PARTS, [smem()] + [vmem()] * 4)(
        place, band_hi, band_lo, *x_parts[2:]
    )
    spectra.append(from_partners(sent))
    weights = call(
        weights_kernel,
        [f32(5, 2, COLS[c], PIX) for c in CHUNKS],
        [smem()] * 3 + [vmem()],
        scratch=[pltpu.VMEM((5, 8, PIX), jnp.float32)] * 2,
    )(place, order_gain, band_shift, sent[0])
    hi0, hi1, lo0, lo1 = call(
        table_kernel,
        [bf16(8 * COLS[c], GRID) for c in CHUNKS] * 2,
        [smem()] + [vmem()] * 2,
    )(place, first, sent[0])
    got = []
    for c in CHUNKS:
        sent = call(
            functools.partial(middle_kernel, c),
            [f32(2 * COLS[c], 2 * ROWS)] * PARTS,
            [smem()] + [vmem()] * 8,
        )(place, *spectra[c], weights[c], y_hi, y_lo, odd)
        got.append(from_partners(sent))
    part = call(part_kernel, f32(2 * ROWS, GRID), [vmem()] * 6)(*got[0], hi0, lo0)
    return call(
        final_kernel,
        f32(2 * ROWS, GRID),
        [vmem()] * 7,
        hbm(),
        [
            pltpu.VMEM((GRID // 128, 2 * ROWS, 128), jnp.float32),
            pltpu.SemaphoreType.DMA((GRID // 128,)),
        ],
    )(*got[1], hi1, lo1, part)


def solution(mesh):
    in_specs = (P("fov", None, "row", None), P("fov"), P("fov", None), P("fov", None))
    out_specs = P(("fov", "row"), None)
    return jax.shard_map(
        reconstruct, mesh=mesh, in_specs=in_specs, out_specs=out_specs, check_vma=False
    )
```

```python
import functools
import math

import jax
import jax.numpy as jnp
import numpy as np
from jax import lax
from jax.experimental import pallas as pl
from jax.experimental.pallas import tpu as pltpu
from jax.sharding import PartitionSpec as P


wiener = 0.1
gain_out = 8.0
cut_share = 0.45
PIX = 512
GRID = 1024
PHASES = 5
PARTS = 4
ROWS = PIX // PARTS
CHUNKS = (0, 1)
LOW = (24, 0)
MAIN = (40, 24)
FOLD_LOW = (24, 16)
FOLD = (40, 8)
COLS = (80, 32)
EXT = (40, 32)
ORDERS = (0, 1, -1, 2, -2)
ARC = (
    1.5707963050,
    -0.2145988016,
    0.0889789874,
    -0.0501743046,
    0.0308918810,
    -0.0170881256,
    0.0066700901,
    -0.0012624911,
)


def split_np(array):
    hi = array.astype(jnp.bfloat16)
    lo = (array - hi.astype(np.float32)).astype(jnp.bfloat16)
    return hi, lo


def split(array):
    hi = array.astype(jnp.bfloat16)
    lo = (array - hi.astype(jnp.float32)).astype(jnp.bfloat16)
    return hi, lo


def column_freq_np(d, chunk):
    def column(low, count):
        l = np.arange(low, low + count)
        return 64 * (l // 16) + 16 * d + l % 16

    fold = column(FOLD_LOW[chunk], FOLD[chunk]) - PIX
    if d == 0 and chunk == 1:
        fold[0] = -PIX // 2
    return np.concatenate([column(LOW[chunk], MAIN[chunk]), fold])


@functools.cache
def tables():
    index = np.arange(PIX)
    angle = 2.0 * np.pi * (np.outer(index[:ROWS], index) % PIX) / PIX
    base = np.stack([np.cos(angle), np.sin(angle)]).astype(np.float32)
    first = np.zeros((PARTS, 2, sum(COLS), 128), np.float32)
    for s in range(PARTS):
        freq = np.concatenate([column_freq_np(s, c) for c in CHUNKS])
        scale = gain_out / (GRID * GRID) * np.where(freq == 0, 1.0, 2.0)
        turn = 2.0 * np.pi * ((freq[:, None] * np.arange(128)[None, :]) % GRID) / GRID
        first[s, 0] = scale[:, None] * np.cos(turn)
        first[s, 1] = scale[:, None] * np.sin(turn)
    turn = 2.0 * np.pi * index / GRID
    odd = np.stack([np.cos(turn), np.sin(turn)]).astype(np.float32)
    return np.stack(split_np(base)), first, odd


def dot3(left, right, dims):
    lhs = jnp.concatenate([left[0], left[0], left[1]], axis=dims[0])
    rhs = jnp.concatenate([right[0], right[1], right[0]], axis=dims[1])
    return lax.dot_general(
        lhs, rhs, (((dims[0],), (dims[1],)), ((), ())), preferred_element_type=jnp.float32
    )


def turn_pair(steps):
    angle = (2.0 * math.pi / PIX) * ((steps + 256) % 512 - 256).astype(jnp.float32)
    return jnp.cos(angle), jnp.sin(angle)


def phase_kernel(place, offset, shift_far, source, base_far, frames, turns, phases, *rest):
    y_out, x_out, (base, shift, sems) = rest[0:2], (rest[2:4], rest[4:6]), rest[6:]
    base_copy = pltpu.make_async_copy(base_far, base, sems.at[0])
    base_copy.start()
    shift_copy = pltpu.make_async_copy(shift_far, shift, sems.at[1])
    shift_copy.start()
    copy = pltpu.make_async_copy(source.at[0], frames, sems.at[2])
    copy.start()
    rank = place[0]
    phase_at = lax.broadcasted_iota(jnp.int32, (8, 128), 0).astype(jnp.float32)
    phase_at = (2.0 * math.pi / PHASES) * phase_at + offset[0]
    phases[0] = jnp.cos(phase_at)
    phases[1] = jnp.sin(phase_at)
    phases[2] = jnp.cos(2.0 * phase_at)
    phases[3] = jnp.sin(2.0 * phase_at)
    lane = lax.broadcasted_iota(jnp.int32, (1, PIX), 1)
    parity = lane % 2
    sign = (1 - lane % 4 + parity).astype(jnp.float32)
    quarter_re = jnp.where(parity == 0, sign, 0.0)
    quarter_im = jnp.where(parity == 1, sign, 0.0)
    half_turn = 1.0 - 2.0 * parity.astype(jnp.float32)
    base_copy.wait()
    for part in range(2):
        cosine, sine = base[part, 0].astype(jnp.float32), base[part, 1].astype(jnp.float32)
        cos_re, cos_im = cosine * quarter_re, cosine * quarter_im
        sin_re, sin_im = sine * quarter_re, sine * quarter_im
        blocks = [
            (cosine, sine),
            (cos_re - sin_im, sin_re + cos_im),
            (cosine * half_turn, sine * half_turn),
            (cos_re + sin_im, sin_re - cos_im),
        ]
        for s in range(PARTS):
            for kind in range(2):
                y_out[part][s, kind] = blocks[s][kind].astype(jnp.bfloat16)
        lone = half_turn if part == 0 else jnp.zeros_like(half_turn)
        top = lax.broadcasted_iota(jnp.int32, (8, PIX), 0) == 0
        for chunk in CHUNKS:
            for d in range(PARTS):
                pieces = []
                for kind in range(2):
                    for l in range(LOW[chunk], LOW[chunk] + MAIN[chunk], 8):
                        column = 64 * (l // 16) + 16 * d + l % 16
                        s, t = column // ROWS, column % ROWS
                        piece = blocks[s][kind][t : t + 8]
                        if column == 0 and kind == 1:
                            piece = jnp.where(top, lone, piece)
                        pieces.append(piece)
                x_out[chunk][part][d] = jnp.concatenate(pieces, axis=0).astype(jnp.bfloat16)
    shift_copy.wait()
    shift_y, shift_x = shift[0:1, 0:1], shift[0:1, 1:2]
    x_cos, x_sin = turn_pair(lax.broadcasted_iota(jnp.int32, (8, PIX), 1) * shift_x)
    row_at = lax.broadcasted_iota(jnp.int32, (ROWS, 128), 0) + rank * ROWS
    y_cos, y_sin = turn_pair(row_at * shift_y)
    x_cos, x_sin = x_cos[:1], x_sin[:1]
    y_cos = jnp.concatenate([y_cos] * 4, axis=1)
    y_sin = jnp.concatenate([y_sin] * 4, axis=1)
    turn_re = x_cos * y_cos - x_sin * y_sin
    turn_im = x_cos * y_sin + x_sin * y_cos
    turns[0] = turn_re
    turns[1] = turn_im
    turns[2] = turn_re * turn_re - turn_im * turn_im
    turns[3] = 2.0 * turn_re * turn_im
    copy.wait()


def spectra_rows(rank, rows, partners, band, x_hi, x_lo, outs):
    table = (
        jnp.concatenate([x_hi[rank ^ k] for k in partners], axis=0),
        jnp.concatenate([x_lo[rank ^ k] for k in partners], axis=0),
    )
    spectra = dot3(table, band, (1, 1))
    for k, out in enumerate(outs):
        for plane in range(5):
            out[plane] = spectra[k * rows : (k + 1) * rows, plane * ROWS : (plane + 1) * ROWS]


def forward_kernel(place, sums0, sums1, sums2, sums3, turns, phases, frames, x_hi, x_lo, *rest):
    outs, (band_hi, band_lo) = rest[:2], rest[2:]
    total = (sums0[...] + sums1[...]) + (sums2[...] + sums3[...])
    weight_all = (PIX * PIX / PHASES) / total
    acc = None
    for p in range(PHASES):
        weight = weight_all[:, p : p + 1]
        plane = frames[p].astype(jnp.float32)
        terms = [plane * weight] + [
            plane * (weight * phases[i, p : p + 1, 0:1]) for i in range(4)
        ]
        acc = terms if p == 0 else [a + b for a, b in zip(acc, terms)]
    zero, one_re, one_im, two_re, two_im = acc
    planes = [
        zero,
        one_re * turns[0] + one_im * turns[1],
        one_re * turns[1] - one_im * turns[0],
        two_re * turns[2] + two_im * turns[3],
        two_re * turns[3] - two_im * turns[2],
    ]
    for index, plane in enumerate(planes):
        hi, lo = split(plane)
        band_hi[index * ROWS : (index + 1) * ROWS, :] = hi
        band_lo[index * ROWS : (index + 1) * ROWS, :] = lo
    band = (band_hi[...], band_lo[...])
    spectra_rows(place[0], 2 * MAIN[0], (2, 3), band, x_hi, x_lo, outs)


def forward_rest_kernel(place, band_hi, band_lo, x_hi0, x_lo0, x_hi1, x_lo1, *outs):
    band = (band_hi[...], band_lo[...])
    spectra_rows(place[0], 2 * MAIN[1], (0, 1, 2, 3), band, x_hi1, x_lo1, outs[2:])
    spectra_rows(place[0], 2 * MAIN[0], (0, 1), band, x_hi0, x_lo0, outs[:2])


def root(value):
    return value * lax.rsqrt(jnp.maximum(value, 1e-30))


def transfer_curve(squared):
    radius = jnp.minimum(root(squared), 1.0)
    arc = jnp.full_like(radius, 2.0 / math.pi * ARC[7])
    for coefficient in ARC[6::-1]:
        arc = arc * radius + 2.0 / math.pi * coefficient
    over = 1.0 + radius
    return root(1.0 - radius) * (arc - (2.0 / math.pi) * radius * (over * lax.rsqrt(over)))


def weights_kernel(chunk, place, gains, shift, after, weights, y_square, y_low):
    rank = place[0]
    shift_y, shift_x = shift[0, 0], shift[0, 1]
    own = [gains[0, m + 2] for m in ORDERS]
    other = [gains[0, 2 - m] for m in ORDERS]
    sub = lax.broadcasted_iota(jnp.int32, (8, 1), 0)
    lane = lax.broadcasted_iota(jnp.int32, (8, PIX), 1)
    for order, m in enumerate(ORDERS):
        y = ((lane - m * shift_y + PIX // 2) & (PIX - 1)) - PIX // 2
        y_low[order] = jnp.where(y + m * shift_y >= 0, 1.0, 0.0)
        y = y.astype(jnp.float32) * (1.0 / (cut_share * PIX))
        y_square[order] = y * y

    def tile_step(tile, carry):
        low = 8 * tile
        folded = low >= MAIN[chunk]
        l = jnp.where(folded, low - MAIN[chunk] + FOLD_LOW[chunk], low + LOW[chunk])
        freq = 64 * (l // 16) + 16 * rank + l % 16
        freq_x = jnp.where(folded, freq - PIX, freq) + sub
        if chunk == 1:
            lone = jnp.logical_and(low == MAIN[1], rank == 0).astype(jnp.int32)
            freq_x = jnp.where(jnp.where(sub == 0, lone, 0) == 1, -PIX // 2, freq_x)
        dens = [jnp.full((8, PIX), wiener, jnp.float32)] * 4
        curves = []
        for order, m in enumerate(ORDERS):
            x = (freq_x - m * shift_x).astype(jnp.float32) * (1.0 / (cut_share * PIX))
            curve = transfer_curve(x * x + y_square[order])
            power = curve * curve
            power_low = power * y_low[order]
            power_high = power - power_low
            g, h = own[order] * own[order], other[order] * other[order]
            dens = [
                dens[0] + g * power_low,
                dens[1] + g * power_high,
                dens[2] + h * power_low,
                dens[3] + h * power_high,
            ]
            curves.append(curve)
        own_low, own_high, other_low, other_high = [0.5 / den for den in dens]
        rows = pl.ds(pl.multiple_of(low, 8), 8)
        for order in range(5):
            is_low = y_low[order] > 0.5
            own_den = jnp.where(is_low, own_low, own_high)
            other_den = jnp.where(is_low, other_low, other_high)
            weight = curves[order] * (own[order] * own_den + other[order] * other_den)
            weights[order, 0, rows, :] = weight
            weights[order, 1, rows, :] = jnp.where(is_low, weight, -weight)

        return carry

    lax.fori_loop(0, COLS[chunk] // 8, tile_step, 0, unroll=2)


def table_kernel(place, first, after, hi0, hi1, lo0, lo1):
    outs = ((hi0, lo0), (hi1, lo1))
    rank = place[0]
    turn = lax.broadcasted_iota(jnp.int32, (8, 128), 0).astype(jnp.float32) * (math.pi / 4)
    turn_re, turn_im = jnp.cos(turn), jnp.sin(turn)
    low = 0
    for chunk in CHUNKS:
        rows = COLS[chunk]
        step_re = jnp.concatenate([turn_re] * (rows // 8), axis=0)
        step_im = jnp.concatenate([turn_im] * (rows // 8), axis=0)
        for k in range(PARTS):
            source = rank ^ k
            re, im = first[source, 0, low : low + rows], first[source, 1, low : low + rows]
            for block in range(GRID // 128):
                lanes = slice(128 * block, 128 * (block + 1))
                for part, value in ((0, re), (1, -im)):
                    at = slice((2 * k + part) * rows, (2 * k + part + 1) * rows)
                    outs[chunk][0][at, lanes], outs[chunk][1][at, lanes] = split(value)
                re, im = re * step_re - im * step_im, re * step_im + im * step_re
        low += rows


def middle_kernel(chunk, place, got0, got1, got2, got3, weights, y_hi, y_lo, odd, *outs):
    rank = place[0]
    blocks = (got0, got1, got2, got3)
    rows, ext, count = COLS[chunk], EXT[chunk], MAIN[chunk]
    if chunk == 1:
        first_row = lax.broadcasted_iota(jnp.int32, (count, PIX), 0) == 0
        lone = jnp.logical_and(first_row, jnp.full((count, PIX), rank, jnp.int32) == 0)
        top = lax.broadcasted_iota(jnp.int32, (8, PIX), 0) == 0
        swap = lone[:8]

    def plane(index):
        whole = jnp.concatenate([b[index] for b in blocks], axis=1)
        cosines, sines = whole[:count], whole[count:]
        if chunk == 0:
            return cosines, sines, None
        return cosines, jnp.where(lone, 0.0, sines), jnp.where(top, sines[:8], 0.0)

    real_rows = []
    imag_rows = []

    def add_row(re, im, extra_re, extra_im):
        real_rows.append(re)
        imag_rows.append(im)
        if chunk == 1:
            real_rows.append(extra_re)
            imag_rows.append(extra_im() if callable(extra_im) else extra_im)

    cos_r, sin_r, extra_r = plane(0)
    add_row(cos_r, -sin_r, extra_r, lambda: jnp.zeros_like(extra_r))
    for m in range(2):
        cos_r, sin_r, extra_r = plane(1 + 2 * m)
        cos_i, sin_i, extra_i = plane(2 + 2 * m)
        add_row(cos_r + sin_i, cos_i - sin_r, extra_r, extra_i)
        add_row(cos_r - sin_i, -cos_i - sin_r, extra_r, lambda: -extra_i)
    data = split(jnp.concatenate(real_rows + imag_rows, axis=0))

    def y_matrix(ref):
        return jnp.concatenate(
            [jnp.concatenate([ref[rank ^ k, 0], ref[rank ^ k, 1]], axis=1) for k in range(PARTS)],
            axis=0,
        )

    turned = dot3(data, (y_matrix(y_hi), y_matrix(y_lo)), (1, 0))
    half = 5 * ext
    spec_re = turned[:half, :PIX] + turned[half:, PIX:]
    spec_im = turned[half:, :PIX] - turned[:half, PIX:]
    sums = None
    for order in range(5):

        def both(spec):
            main = spec[order * ext : order * ext + count]
            if chunk == 0:
                return jnp.concatenate([main, main], axis=0)
            extra = spec[order * ext + count : (order + 1) * ext]
            return jnp.concatenate(
                [main, jnp.where(swap, extra, main[16:24])] + ([main[24:]] if count > 24 else []), axis=0
            )

        re, im = both(spec_re), both(spec_im)
        plus, minus = weights[order, 0], weights[order, 1]
        terms = (plus * re, plus * im, minus * re, minus * im)
        sums = terms if order == 0 else tuple(a + b for a, b in zip(sums, terms))
    even_re, even_im, odd_re, odd_im = sums
    odd_cos, odd_sin = odd[0:1], odd[1:2]
    odd_re, odd_im = odd_re * odd_cos - odd_im * odd_sin, odd_re * odd_sin + odd_im * odd_cos
    filtered = split(jnp.concatenate([even_re, even_im, odd_re, odd_im], axis=0))

    def u_matrix(ref):
        return jnp.concatenate(
            [jnp.concatenate([ref[rank ^ k, 0], ref[rank ^ k, 1]], axis=0) for k in range(PARTS)],
            axis=0,
        )

    back = dot3(filtered, (u_matrix(y_hi), u_matrix(y_lo)), (1, 1))
    for k in range(PARTS):
        cos_part = back[:, 2 * ROWS * k : 2 * ROWS * k + ROWS]
        sin_part = back[:, 2 * ROWS * k + ROWS : 2 * ROWS * (k + 1)]
        for parity in range(2):
            base = 2 * rows * parity
            re, im = slice(base, base + rows), slice(base + rows, base + 2 * rows)
            lanes = slice(parity * ROWS, (parity + 1) * ROWS)
            outs[k][0:rows, lanes] = cos_part[re] - sin_part[im]
            outs[k][rows : 2 * rows, lanes] = sin_part[re] + cos_part[im]


def gathered(blocks):
    return split(jnp.concatenate([b[...] for b in blocks], axis=0))


def part_kernel(got0, got1, got2, got3, final_hi, final_lo, part):
    data = gathered((got0, got1, got2, got3))
    part[...] = dot3(data, (final_hi[...], final_lo[...]), (0, 0))


def final_kernel(got0, got1, got2, got3, final_hi, final_lo, part, out, woven, sems):
    data = gathered((got0, got1, got2, got3))
    copies = []
    for strip in range(GRID // 256):
        lanes = slice(256 * strip, 256 * (strip + 1))
        picture = part[:, lanes] + dot3(data, (final_hi[:, lanes], final_lo[:, lanes]), (0, 0))
        for block in range(2):
            at = 2 * strip + block
            piece = slice(128 * block, 128 * (block + 1))
            woven[at, pl.ds(0, ROWS, 2), :] = picture[:ROWS, piece]
            woven[at, pl.ds(1, ROWS, 2), :] = picture[ROWS:, piece]
            copy = pltpu.make_async_copy(
                woven.at[at], out.at[:, pl.ds(128 * at, 128)], sems.at[at]
            )
            copy.start()
            copies.append(copy)
    for copy in copies:
        copy.wait()


def smem():
    return pl.BlockSpec(memory_space=pltpu.SMEM)


def vmem():
    return pl.BlockSpec(memory_space=pltpu.VMEM)


def hbm():
    return pl.BlockSpec(memory_space=pltpu.HBM)


def f32(*shape):
    return jax.ShapeDtypeStruct(shape, jnp.float32)


def bf16(*shape):
    return jax.ShapeDtypeStruct(shape, jnp.bfloat16)


def call(kernel, out_shape, in_specs, out_specs=None, scratch=(), limit=24):
    if out_specs is None:
        out_specs = jax.tree.map(lambda _: vmem(), out_shape)
    return pl.pallas_call(
        kernel,
        out_shape=out_shape,
        in_specs=in_specs,
        out_specs=out_specs,
        scratch_shapes=list(scratch),
        compiler_params=pltpu.CompilerParams(vmem_limit_bytes=limit * 1024 * 1024),
    )


def from_partners(blocks):
    got = [blocks[0]]
    for k in range(1, PARTS):
        got.append(lax.ppermute(blocks[k], "row", [(i, i ^ k) for i in range(PARTS)]))
    return got


def reconstruct(frames, phase_offset, order_gain, band_shift):
    base, first, odd = tables()
    rank = lax.axis_index("row")
    place = rank.reshape(1).astype(jnp.int32)

    sums = jnp.sum(frames.astype(jnp.float32), axis=(2, 3))
    sums = from_partners([sums] * PARTS)
    frames, turns, phases, y_hi, y_lo, *x_parts = call(
        phase_kernel,
        [bf16(PHASES, ROWS, PIX), f32(4, ROWS, PIX), f32(4, 8, 128)]
        + [bf16(PARTS, 2, ROWS, PIX)] * 2
        + [bf16(PARTS, 2 * MAIN[c], PIX) for c in CHUNKS for _ in range(2)],
        [smem()] * 2 + [hbm()] * 3,
        scratch=[
            pltpu.VMEM(base.shape, jnp.bfloat16),
            pltpu.VMEM((1, 2), jnp.int32),
            pltpu.SemaphoreType.DMA((3,)),
        ],
    )(
        place,
        phase_offset,
        pltpu.with_memory_space_constraint(band_shift, pltpu.HBM),
        pltpu.with_memory_space_constraint(frames, pltpu.HBM),
        pltpu.with_memory_space_constraint(base, pltpu.HBM),
    )
    blocks = [f32(5, 2 * MAIN[c], ROWS) for c in CHUNKS]
    *far, band_hi, band_lo = call(
        forward_kernel,
        [blocks[0]] * 2 + [bf16(5 * ROWS, PIX)] * 2,
        [smem()] + [vmem()] * 9,
    )(place, *sums, turns, phases, frames, *x_parts[:2])
    sent = call(
        forward_rest_kernel,
        [blocks[0]] * 2 + [blocks[1]] * PARTS,
        [smem()] + [vmem()] * 6,
    )(place, band_hi, band_lo, *x_parts)
    spectra = [from_partners([*sent[:2], *far]), from_partners(sent[2:])]
    got = []
    after = sent[0]
    for c in CHUNKS:
        weights = call(
            functools.partial(weights_kernel, c),
            f32(5, 2, COLS[c], PIX),
            [smem()] * 3 + [vmem()],
            scratch=[pltpu.VMEM((5, 8, PIX), jnp.float32)] * 2,
        )(place, order_gain, band_shift, after)
        sent = call(
            functools.partial(middle_kernel, c),
            [f32(2 * COLS[c], 2 * ROWS)] * PARTS,
            [smem()] + [vmem()] * 8,
        )(place, *spectra[c], weights, y_hi, y_lo, odd)
        after = sent[0]
        got.append(from_partners(sent))
    hi0, hi1, lo0, lo1 = call(
        table_kernel,
        [bf16(8 * COLS[c], GRID) for c in CHUNKS] * 2,
        [smem()] + [vmem()] * 2,
    )(place, first, after)
    part = call(part_kernel, f32(2 * ROWS, GRID), [vmem()] * 6)(*got[0], hi0, lo0)
    return call(
        final_kernel,
        f32(2 * ROWS, GRID),
        [vmem()] * 7,
        hbm(),
        [
            pltpu.VMEM((GRID // 128, 2 * ROWS, 128), jnp.float32),
            pltpu.SemaphoreType.DMA((GRID // 128,)),
        ],
    )(*got[1], hi1, lo1, part)


def solution(mesh):
    in_specs = (P("fov", None, "row", None), P("fov"), P("fov", None), P("fov", None))
    out_specs = P(("fov", "row"), None)
    return jax.shard_map(
        reconstruct, mesh=mesh, in_specs=in_specs, out_specs=out_specs, check_vma=False
    )
```

```python
import functools
import math

import jax
import jax.numpy as jnp
import numpy as np
from jax import lax
from jax.experimental import pallas as pl
from jax.experimental.pallas import tpu as pltpu
from jax.sharding import PartitionSpec as P


wiener = 0.1
gain_out = 8.0
cut_share = 0.45
PIX = 512
GRID = 1024
PHASES = 5
PARTS = 4
ROWS = PIX // PARTS
CHUNKS = (0, 1)
LOW = (32, 0)
MAIN = (32, 32)
FOLD_LOW = (32, 16)
FOLD = (32, 16)
COLS = (64, 48)
EXT = (32, 40)
ORDERS = (0, 1, -1, 2, -2)
ARC = (
    1.5707963050,
    -0.2145988016,
    0.0889789874,
    -0.0501743046,
    0.0308918810,
    -0.0170881256,
    0.0066700901,
    -0.0012624911,
)


def split_np(array):
    hi = array.astype(jnp.bfloat16)
    lo = (array - hi.astype(np.float32)).astype(jnp.bfloat16)
    return hi, lo


def split(array):
    hi = array.astype(jnp.bfloat16)
    lo = (array - hi.astype(jnp.float32)).astype(jnp.bfloat16)
    return hi, lo


def column_freq_np(d, chunk):
    def column(low, count):
        l = np.arange(low, low + count)
        return 64 * (l // 16) + 16 * d + l % 16

    fold = column(FOLD_LOW[chunk], FOLD[chunk]) - PIX
    if d == 0 and chunk == 1:
        fold[0] = -PIX // 2
    return np.concatenate([column(LOW[chunk], MAIN[chunk]), fold])


@functools.cache
def tables():
    index = np.arange(PIX)
    angle = 2.0 * np.pi * (np.outer(index[:ROWS], index) % PIX) / PIX
    base = np.stack([np.cos(angle), np.sin(angle)]).astype(np.float32)
    first = np.zeros((PARTS, 2, sum(COLS), 128), np.float32)
    for s in range(PARTS):
        freq = np.concatenate([column_freq_np(s, c) for c in CHUNKS])
        scale = gain_out / (GRID * GRID) * np.where(freq == 0, 1.0, 2.0)
        turn = 2.0 * np.pi * ((freq[:, None] * np.arange(128)[None, :]) % GRID) / GRID
        first[s, 0] = scale[:, None] * np.cos(turn)
        first[s, 1] = scale[:, None] * np.sin(turn)
    turn = 2.0 * np.pi * index / GRID
    odd = np.stack([np.cos(turn), np.sin(turn)]).astype(np.float32)
    return np.stack(split_np(base)), first, odd


def dot3(left, right, dims):
    lhs = jnp.concatenate([left[0], left[0], left[1]], axis=dims[0])
    rhs = jnp.concatenate([right[0], right[1], right[0]], axis=dims[1])
    return lax.dot_general(
        lhs, rhs, (((dims[0],), (dims[1],)), ((), ())), preferred_element_type=jnp.float32
    )


def turn_pair(steps):
    angle = (2.0 * math.pi / PIX) * ((steps + 256) % 512 - 256).astype(jnp.float32)
    return jnp.cos(angle), jnp.sin(angle)


def row_blocks(base, part, count):
    lane = lax.broadcasted_iota(jnp.int32, (1, PIX), 1)
    parity = lane % 2
    sign = (1 - lane % 4 + parity).astype(jnp.float32)
    quarter_re = jnp.where(parity == 0, sign, 0.0)
    quarter_im = jnp.where(parity == 1, sign, 0.0)
    half_turn = 1.0 - 2.0 * parity.astype(jnp.float32)
    cosine, sine = base[part, 0].astype(jnp.float32), base[part, 1].astype(jnp.float32)
    cos_re, cos_im = cosine * quarter_re, cosine * quarter_im
    sin_re, sin_im = sine * quarter_re, sine * quarter_im
    blocks = [(cosine, sine), (cos_re - sin_im, sin_re + cos_im)]
    if count > 2:
        blocks += [
            (cosine * half_turn, sine * half_turn),
            (cos_re + sin_im, sin_re - cos_im),
        ]
    return blocks, half_turn


def x_rows(base, chunk, outs):
    top = lax.broadcasted_iota(jnp.int32, (8, PIX), 0) == 0
    for part in range(2):
        blocks, half_turn = row_blocks(base, part, 2)
        lone = half_turn if part == 0 else jnp.zeros_like(half_turn)
        for d in range(PARTS):
            pieces = []
            for kind in range(2):
                for l in range(LOW[chunk], LOW[chunk] + MAIN[chunk], 8):
                    column = 64 * (l // 16) + 16 * d + l % 16
                    s, t = column // ROWS, column % ROWS
                    piece = blocks[s][kind][t : t + 8]
                    if column == 0 and kind == 1:
                        piece = jnp.where(top, lone, piece)
                    pieces.append(piece)
            outs[part][d] = jnp.concatenate(pieces, axis=0).astype(jnp.bfloat16)


def phase_kernel(
    place, offset, shift_far, source, base_far, frames, turns, phases, base, x_hi, x_lo, shift, sems
):
    base_copy = pltpu.make_async_copy(base_far, base, sems.at[0])
    base_copy.start()
    shift_copy = pltpu.make_async_copy(shift_far, shift, sems.at[1])
    shift_copy.start()
    copy = pltpu.make_async_copy(source.at[0], frames, sems.at[2])
    copy.start()
    rank = place[0]
    phase_at = lax.broadcasted_iota(jnp.int32, (8, 128), 0).astype(jnp.float32)
    phase_at = (2.0 * math.pi / PHASES) * phase_at + offset[0]
    phases[0] = jnp.cos(phase_at)
    phases[1] = jnp.sin(phase_at)
    phases[2] = jnp.cos(2.0 * phase_at)
    phases[3] = jnp.sin(2.0 * phase_at)
    shift_copy.wait()
    shift_y, shift_x = shift[0:1, 0:1], shift[0:1, 1:2]
    x_cos, x_sin = turn_pair(lax.broadcasted_iota(jnp.int32, (8, PIX), 1) * shift_x)
    row_at = lax.broadcasted_iota(jnp.int32, (ROWS, 128), 0) + rank * ROWS
    y_cos, y_sin = turn_pair(row_at * shift_y)
    x_cos, x_sin = x_cos[:1], x_sin[:1]
    y_cos = jnp.concatenate([y_cos] * 4, axis=1)
    y_sin = jnp.concatenate([y_sin] * 4, axis=1)
    turn_re = x_cos * y_cos - x_sin * y_sin
    turn_im = x_cos * y_sin + x_sin * y_cos
    turns[0] = turn_re
    turns[1] = turn_im
    turns[2] = turn_re * turn_re - turn_im * turn_im
    turns[3] = 2.0 * turn_re * turn_im
    base_copy.wait()
    x_rows(base, 0, (x_hi, x_lo))
    copy.wait()


def spectra_rows(rank, rows, partners, band, x_hi, x_lo, outs):
    table = (
        jnp.concatenate([x_hi[rank ^ k] for k in partners], axis=0),
        jnp.concatenate([x_lo[rank ^ k] for k in partners], axis=0),
    )
    spectra = dot3(table, band, (1, 1))
    for k, out in enumerate(outs):
        for plane in range(5):
            out[plane] = spectra[k * rows : (k + 1) * rows, plane * ROWS : (plane + 1) * ROWS]


def forward_kernel(place, sums0, sums1, sums2, sums3, turns, phases, frames, x_hi, x_lo, *rest):
    outs, (band_hi, band_lo) = rest[:2], rest[2:]
    total = (sums0[...] + sums1[...]) + (sums2[...] + sums3[...])
    weight_all = (PIX * PIX / PHASES) / total
    acc = None
    for p in range(PHASES):
        weight = weight_all[:, p : p + 1]
        plane = frames[p].astype(jnp.float32)
        terms = [plane * weight] + [
            plane * (weight * phases[i, p : p + 1, 0:1]) for i in range(4)
        ]
        acc = terms if p == 0 else [a + b for a, b in zip(acc, terms)]
    zero, one_re, one_im, two_re, two_im = acc
    planes = [
        zero,
        one_re * turns[0] + one_im * turns[1],
        one_re * turns[1] - one_im * turns[0],
        two_re * turns[2] + two_im * turns[3],
        two_re * turns[3] - two_im * turns[2],
    ]
    for index, plane in enumerate(planes):
        hi, lo = split(plane)
        band_hi[index * ROWS : (index + 1) * ROWS, :] = hi
        band_lo[index * ROWS : (index + 1) * ROWS, :] = lo
    band = (band_hi[...], band_lo[...])
    spectra_rows(place[0], 2 * MAIN[0], (2, 3), band, x_hi, x_lo, outs)


def forward_rest_kernel(place, band_hi, band_lo, x_hi0, x_lo0, base, *rest):
    outs, (y_hi, y_lo, x_hi1, x_lo1) = rest[:6], rest[6:]
    x_rows(base, 1, (x_hi1, x_lo1))
    band = (band_hi[...], band_lo[...])
    spectra_rows(place[0], 2 * MAIN[1], (0, 1, 2, 3), band, x_hi1, x_lo1, outs[2:])
    spectra_rows(place[0], 2 * MAIN[0], (0, 1), band, x_hi0, x_lo0, outs[:2])
    for part, out in ((0, y_hi), (1, y_lo)):
        blocks, _ = row_blocks(base, part, PARTS)
        for s in range(PARTS):
            for kind in range(2):
                out[s, kind] = blocks[s][kind].astype(jnp.bfloat16)


def root(value):
    return value * lax.rsqrt(jnp.maximum(value, 1e-30))


def transfer_curve(squared):
    radius = jnp.minimum(root(squared), 1.0)
    arc = jnp.full_like(radius, 2.0 / math.pi * ARC[7])
    for coefficient in ARC[6::-1]:
        arc = arc * radius + 2.0 / math.pi * coefficient
    over = 1.0 + radius
    return root(1.0 - radius) * (arc - (2.0 / math.pi) * radius * (over * lax.rsqrt(over)))


def weights_kernel(chunk, place, gains, shift, after, weights, y_square, y_low):
    rank = place[0]
    shift_y, shift_x = shift[0, 0], shift[0, 1]
    own = [gains[0, m + 2] for m in ORDERS]
    other = [gains[0, 2 - m] for m in ORDERS]
    sub = lax.broadcasted_iota(jnp.int32, (8, 1), 0)
    lane = lax.broadcasted_iota(jnp.int32, (8, PIX), 1)
    for order, m in enumerate(ORDERS):
        y = ((lane - m * shift_y + PIX // 2) & (PIX - 1)) - PIX // 2
        y_low[order] = jnp.where(y + m * shift_y >= 0, 1.0, 0.0)
        y = y.astype(jnp.float32) * (1.0 / (cut_share * PIX))
        y_square[order] = y * y

    def tile_step(tile, carry):
        low = 8 * tile
        folded = low >= MAIN[chunk]
        l = jnp.where(folded, low - MAIN[chunk] + FOLD_LOW[chunk], low + LOW[chunk])
        freq = 64 * (l // 16) + 16 * rank + l % 16
        freq_x = jnp.where(folded, freq - PIX, freq) + sub
        if chunk == 1:
            lone = jnp.logical_and(low == MAIN[1], rank == 0).astype(jnp.int32)
            freq_x = jnp.where(jnp.where(sub == 0, lone, 0) == 1, -PIX // 2, freq_x)
        dens = [jnp.full((8, PIX), wiener, jnp.float32)] * 4
        curves = []
        for order, m in enumerate(ORDERS):
            x = (freq_x - m * shift_x).astype(jnp.float32) * (1.0 / (cut_share * PIX))
            curve = transfer_curve(x * x + y_square[order])
            power = curve * curve
            power_low = power * y_low[order]
            power_high = power - power_low
            g, h = own[order] * own[order], other[order] * other[order]
            dens = [
                dens[0] + g * power_low,
                dens[1] + g * power_high,
                dens[2] + h * power_low,
                dens[3] + h * power_high,
            ]
            curves.append(curve)
        own_low, own_high, other_low, other_high = [0.5 / den for den in dens]
        rows = pl.ds(pl.multiple_of(low, 8), 8)
        for order in range(5):
            is_low = y_low[order] > 0.5
            own_den = jnp.where(is_low, own_low, own_high)
            other_den = jnp.where(is_low, other_low, other_high)
            weight = curves[order] * (own[order] * own_den + other[order] * other_den)
            weights[order, 0, rows, :] = weight
            weights[order, 1, rows, :] = jnp.where(is_low, weight, -weight)

        return carry

    lax.fori_loop(0, COLS[chunk] // 8, tile_step, 0, unroll=2)


def table_kernel(place, first, after, hi0, hi1, lo0, lo1):
    outs = ((hi0, lo0), (hi1, lo1))
    rank = place[0]
    turn = lax.broadcasted_iota(jnp.int32, (8, 128), 0).astype(jnp.float32) * (math.pi / 4)
    turn_re, turn_im = jnp.cos(turn), jnp.sin(turn)
    low = 0
    for chunk in CHUNKS:
        rows = COLS[chunk]
        step_re = jnp.concatenate([turn_re] * (rows // 8), axis=0)
        step_im = jnp.concatenate([turn_im] * (rows // 8), axis=0)
        for k in range(PARTS):
            source = rank ^ k
            re, im = first[source, 0, low : low + rows], first[source, 1, low : low + rows]
            for block in range(GRID // 128):
                lanes = slice(128 * block, 128 * (block + 1))
                for part, value in ((0, re), (1, -im)):
                    at = slice((2 * k + part) * rows, (2 * k + part + 1) * rows)
                    outs[chunk][0][at, lanes], outs[chunk][1][at, lanes] = split(value)
                re, im = re * step_re - im * step_im, re * step_im + im * step_re
        low += rows


def middle_kernel(chunk, place, got0, got1, got2, got3, weights, y_hi, y_lo, odd, *outs):
    rank = place[0]
    blocks = (got0, got1, got2, got3)
    rows, ext, count = COLS[chunk], EXT[chunk], MAIN[chunk]
    if chunk == 1:
        first_row = lax.broadcasted_iota(jnp.int32, (count, PIX), 0) == 0
        lone = jnp.logical_and(first_row, jnp.full((count, PIX), rank, jnp.int32) == 0)
        top = lax.broadcasted_iota(jnp.int32, (8, PIX), 0) == 0
        swap = lone[:8]

    def plane(index):
        whole = jnp.concatenate([b[index] for b in blocks], axis=1)
        cosines, sines = whole[:count], whole[count:]
        if chunk == 0:
            return cosines, sines, None
        return cosines, jnp.where(lone, 0.0, sines), jnp.where(top, sines[:8], 0.0)

    real_rows = []
    imag_rows = []

    def add_row(re, im, extra_re, extra_im):
        real_rows.append(re)
        imag_rows.append(im)
        if chunk == 1:
            real_rows.append(extra_re)
            imag_rows.append(extra_im() if callable(extra_im) else extra_im)

    cos_r, sin_r, extra_r = plane(0)
    add_row(cos_r, -sin_r, extra_r, lambda: jnp.zeros_like(extra_r))
    for m in range(2):
        cos_r, sin_r, extra_r = plane(1 + 2 * m)
        cos_i, sin_i, extra_i = plane(2 + 2 * m)
        add_row(cos_r + sin_i, cos_i - sin_r, extra_r, extra_i)
        add_row(cos_r - sin_i, -cos_i - sin_r, extra_r, lambda: -extra_i)
    data = split(jnp.concatenate(real_rows + imag_rows, axis=0))

    def y_matrix(ref):
        return jnp.concatenate(
            [jnp.concatenate([ref[rank ^ k, 0], ref[rank ^ k, 1]], axis=1) for k in range(PARTS)],
            axis=0,
        )

    turned = dot3(data, (y_matrix(y_hi), y_matrix(y_lo)), (1, 0))
    half = 5 * ext
    spec_re = turned[:half, :PIX] + turned[half:, PIX:]
    spec_im = turned[half:, :PIX] - turned[:half, PIX:]
    sums = None
    for order in range(5):

        def both(spec):
            main = spec[order * ext : order * ext + count]
            if chunk == 0:
                return jnp.concatenate([main, main], axis=0)
            extra = spec[order * ext + count : (order + 1) * ext]
            return jnp.concatenate(
                [main, jnp.where(swap, extra, main[16:24])] + ([main[24:]] if count > 24 else []), axis=0
            )

        re, im = both(spec_re), both(spec_im)
        plus, minus = weights[order, 0], weights[order, 1]
        terms = (plus * re, plus * im, minus * re, minus * im)
        sums = terms if order == 0 else tuple(a + b for a, b in zip(sums, terms))
    even_re, even_im, odd_re, odd_im = sums
    odd_cos, odd_sin = odd[0:1], odd[1:2]
    odd_re, odd_im = odd_re * odd_cos - odd_im * odd_sin, odd_re * odd_sin + odd_im * odd_cos
    filtered = split(jnp.concatenate([even_re, even_im, odd_re, odd_im], axis=0))

    def u_matrix(ref):
        return jnp.concatenate(
            [jnp.concatenate([ref[rank ^ k, 0], ref[rank ^ k, 1]], axis=0) for k in range(PARTS)],
            axis=0,
        )

    back = dot3(filtered, (u_matrix(y_hi), u_matrix(y_lo)), (1, 1))
    for k in range(PARTS):
        cos_part = back[:, 2 * ROWS * k : 2 * ROWS * k + ROWS]
        sin_part = back[:, 2 * ROWS * k + ROWS : 2 * ROWS * (k + 1)]
        for parity in range(2):
            base = 2 * rows * parity
            re, im = slice(base, base + rows), slice(base + rows, base + 2 * rows)
            lanes = slice(parity * ROWS, (parity + 1) * ROWS)
            outs[k][0:rows, lanes] = cos_part[re] - sin_part[im]
            outs[k][rows : 2 * rows, lanes] = sin_part[re] + cos_part[im]


def gathered(blocks):
    return split(jnp.concatenate([b[...] for b in blocks], axis=0))


def part_kernel(got0, got1, got2, got3, final_hi, final_lo, part):
    data = gathered((got0, got1, got2, got3))
    part[...] = dot3(data, (final_hi[...], final_lo[...]), (0, 0))


def final_kernel(got0, got1, got2, got3, final_hi, final_lo, part, out, woven, sems):
    data = gathered((got0, got1, got2, got3))
    copies = []
    for strip in range(GRID // 256):
        lanes = slice(256 * strip, 256 * (strip + 1))
        picture = part[:, lanes] + dot3(data, (final_hi[:, lanes], final_lo[:, lanes]), (0, 0))
        for block in range(2):
            at = 2 * strip + block
            piece = slice(128 * block, 128 * (block + 1))
            woven[at, pl.ds(0, ROWS, 2), :] = picture[:ROWS, piece]
            woven[at, pl.ds(1, ROWS, 2), :] = picture[ROWS:, piece]
            copy = pltpu.make_async_copy(
                woven.at[at], out.at[:, pl.ds(128 * at, 128)], sems.at[at]
            )
            copy.start()
            copies.append(copy)
    for copy in copies:
        copy.wait()


def smem():
    return pl.BlockSpec(memory_space=pltpu.SMEM)


def vmem():
    return pl.BlockSpec(memory_space=pltpu.VMEM)


def hbm():
    return pl.BlockSpec(memory_space=pltpu.HBM)


def f32(*shape):
    return jax.ShapeDtypeStruct(shape, jnp.float32)


def bf16(*shape):
    return jax.ShapeDtypeStruct(shape, jnp.bfloat16)


def call(kernel, out_shape, in_specs, out_specs=None, scratch=(), limit=24):
    if out_specs is None:
        out_specs = jax.tree.map(lambda _: vmem(), out_shape)
    return pl.pallas_call(
        kernel,
        out_shape=out_shape,
        in_specs=in_specs,
        out_specs=out_specs,
        scratch_shapes=list(scratch),
        compiler_params=pltpu.CompilerParams(vmem_limit_bytes=limit * 1024 * 1024),
    )


def from_partners(blocks):
    got = [blocks[0]]
    for k in range(1, PARTS):
        got.append(lax.ppermute(blocks[k], "row", [(i, i ^ k) for i in range(PARTS)]))
    return got


def reconstruct(frames, phase_offset, order_gain, band_shift):
    base, first, odd = tables()
    rank = lax.axis_index("row")
    place = rank.reshape(1).astype(jnp.int32)

    sums = jnp.sum(frames.astype(jnp.float32), axis=(2, 3))
    sums = from_partners([sums] * PARTS)
    table = bf16(PARTS, 2 * MAIN[0], PIX)
    frames, turns, phases, near_base, *x_parts = call(
        phase_kernel,
        [bf16(PHASES, ROWS, PIX), f32(4, ROWS, PIX), f32(4, 8, 128), bf16(*base.shape)]
        + [table] * 2,
        [smem()] * 2 + [hbm()] * 3,
        scratch=[pltpu.VMEM((1, 2), jnp.int32), pltpu.SemaphoreType.DMA((3,))],
    )(
        place,
        phase_offset,
        pltpu.with_memory_space_constraint(band_shift, pltpu.HBM),
        pltpu.with_memory_space_constraint(frames, pltpu.HBM),
        pltpu.with_memory_space_constraint(base, pltpu.HBM),
    )
    blocks = [f32(5, 2 * MAIN[c], ROWS) for c in CHUNKS]
    *far, band_hi, band_lo = call(
        forward_kernel,
        [blocks[0]] * 2 + [bf16(5 * ROWS, PIX)] * 2,
        [smem()] + [vmem()] * 9,
    )(place, *sums, turns, phases, frames, *x_parts)
    *sent, y_hi, y_lo = call(
        forward_rest_kernel,
        [blocks[0]] * 2 + [blocks[1]] * PARTS + [bf16(PARTS, 2, ROWS, PIX)] * 2,
        [smem()] + [vmem()] * 5,
        scratch=[pltpu.VMEM((PARTS, 2 * MAIN[1], PIX), jnp.bfloat16)] * 2,
    )(place, band_hi, band_lo, *x_parts, near_base)
    spectra = [from_partners([*sent[:2], *far]), from_partners(sent[2:])]
    got = []
    after = sent[0]
    for c in CHUNKS:
        weights = call(
            functools.partial(weights_kernel, c),
            f32(5, 2, COLS[c], PIX),
            [smem()] * 3 + [vmem()],
            scratch=[pltpu.VMEM((5, 8, PIX), jnp.float32)] * 2,
        )(place, order_gain, band_shift, after)
        sent = call(
            functools.partial(middle_kernel, c),
            [f32(2 * COLS[c], 2 * ROWS)] * PARTS,
            [smem()] + [vmem()] * 8,
        )(place, *spectra[c], weights, y_hi, y_lo, odd)
        after = sent[0]
        got.append(from_partners(sent))
    hi0, hi1, lo0, lo1 = call(
        table_kernel,
        [bf16(8 * COLS[c], GRID) for c in CHUNKS] * 2,
        [smem()] + [vmem()] * 2,
    )(place, first, after)
    part = call(part_kernel, f32(2 * ROWS, GRID), [vmem()] * 6)(*got[0], hi0, lo0)
    return call(
        final_kernel,
        f32(2 * ROWS, GRID),
        [vmem()] * 7,
        hbm(),
        [
            pltpu.VMEM((GRID // 128, 2 * ROWS, 128), jnp.float32),
            pltpu.SemaphoreType.DMA((GRID // 128,)),
        ],
    )(*got[1], hi1, lo1, part)


def solution(mesh):
    in_specs = (P("fov", None, "row", None), P("fov"), P("fov", None), P("fov", None))
    out_specs = P(("fov", "row"), None)
    return jax.shard_map(
        reconstruct, mesh=mesh, in_specs=in_specs, out_specs=out_specs, check_vma=False
    )
```

```python
import functools
import math

import jax
import jax.numpy as jnp
import numpy as np
from jax import lax
from jax.experimental import pallas as pl
from jax.experimental.pallas import tpu as pltpu
from jax.sharding import PartitionSpec as P


wiener = 0.1
gain_out = 8.0
cut_share = 0.45
PIX = 512
GRID = 1024
PHASES = 5
PARTS = 4
ROWS = PIX // PARTS
CHUNKS = (0, 1)
LOW = (24, 0)
MAIN = (40, 24)
FOLD_LOW = (24, 16)
FOLD = (40, 8)
COLS = (80, 32)
EXT = (40, 32)
ORDERS = (0, 1, -1, 2, -2)
ARC = (
    1.5707963050,
    -0.2145988016,
    0.0889789874,
    -0.0501743046,
    0.0308918810,
    -0.0170881256,
    0.0066700901,
    -0.0012624911,
)


def split_np(array):
    hi = array.astype(jnp.bfloat16)
    lo = (array - hi.astype(np.float32)).astype(jnp.bfloat16)
    return hi, lo


def split(array):
    hi = array.astype(jnp.bfloat16)
    lo = (array - hi.astype(jnp.float32)).astype(jnp.bfloat16)
    return hi, lo


def column_freq_np(d, chunk):
    def column(low, count):
        l = np.arange(low, low + count)
        return 64 * (l // 16) + 16 * d + l % 16

    fold = column(FOLD_LOW[chunk], FOLD[chunk]) - PIX
    if d == 0 and chunk == 1:
        fold[0] = -PIX // 2
    return np.concatenate([column(LOW[chunk], MAIN[chunk]), fold])


@functools.cache
def tables():
    index = np.arange(PIX)
    angle = 2.0 * np.pi * (np.outer(index[:ROWS], index) % PIX) / PIX
    base = np.stack([np.cos(angle), np.sin(angle)]).astype(np.float32)
    first = np.zeros((PARTS, 2, sum(COLS), 128), np.float32)
    for s in range(PARTS):
        freq = np.concatenate([column_freq_np(s, c) for c in CHUNKS])
        scale = gain_out / (GRID * GRID) * np.where(freq == 0, 1.0, 2.0)
        turn = 2.0 * np.pi * ((freq[:, None] * np.arange(128)[None, :]) % GRID) / GRID
        first[s, 0] = scale[:, None] * np.cos(turn)
        first[s, 1] = scale[:, None] * np.sin(turn)
    turn = 2.0 * np.pi * index / GRID
    odd = np.stack([np.cos(turn), np.sin(turn)]).astype(np.float32)
    return np.stack(split_np(base)), first, odd


def dot3(left, right, dims):
    lhs = jnp.concatenate([left[0], left[0], left[1]], axis=dims[0])
    rhs = jnp.concatenate([right[0], right[1], right[0]], axis=dims[1])
    return lax.dot_general(
        lhs, rhs, (((dims[0],), (dims[1],)), ((), ())), preferred_element_type=jnp.float32
    )


def turn_pair(steps):
    angle = (2.0 * math.pi / PIX) * ((steps + 256) % 512 - 256).astype(jnp.float32)
    return jnp.cos(angle), jnp.sin(angle)


def row_blocks(base, part, count):
    lane = lax.broadcasted_iota(jnp.int32, (1, PIX), 1)
    parity = lane % 2
    sign = (1 - lane % 4 + parity).astype(jnp.float32)
    quarter_re = jnp.where(parity == 0, sign, 0.0)
    quarter_im = jnp.where(parity == 1, sign, 0.0)
    half_turn = 1.0 - 2.0 * parity.astype(jnp.float32)
    cosine, sine = base[part, 0].astype(jnp.float32), base[part, 1].astype(jnp.float32)
    cos_re, cos_im = cosine * quarter_re, cosine * quarter_im
    sin_re, sin_im = sine * quarter_re, sine * quarter_im
    blocks = [(cosine, sine), (cos_re - sin_im, sin_re + cos_im)]
    if count > 2:
        blocks += [
            (cosine * half_turn, sine * half_turn),
            (cos_re + sin_im, sin_re - cos_im),
        ]
    return blocks, half_turn


def x_rows(base, chunk, outs):
    top = lax.broadcasted_iota(jnp.int32, (8, PIX), 0) == 0
    for part in range(2):
        blocks, half_turn = row_blocks(base, part, 2)
        lone = half_turn if part == 0 else jnp.zeros_like(half_turn)
        for d in range(PARTS):
            pieces = []
            for kind in range(2):
                for l in range(LOW[chunk], LOW[chunk] + MAIN[chunk], 8):
                    column = 64 * (l // 16) + 16 * d + l % 16
                    s, t = column // ROWS, column % ROWS
                    piece = blocks[s][kind][t : t + 8]
                    if column == 0 and kind == 1:
                        piece = jnp.where(top, lone, piece)
                    pieces.append(piece)
            outs[part][d] = jnp.concatenate(pieces, axis=0).astype(jnp.bfloat16)


def phase_kernel(
    place, offset, shift_far, source, base_far, frames, turns, phases, base, x_hi, x_lo, shift, sems
):
    base_copy = pltpu.make_async_copy(base_far, base, sems.at[0])
    base_copy.start()
    shift_copy = pltpu.make_async_copy(shift_far, shift, sems.at[1])
    shift_copy.start()
    copy = pltpu.make_async_copy(source.at[0], frames, sems.at[2])
    copy.start()
    rank = place[0]
    phase_at = lax.broadcasted_iota(jnp.int32, (8, 128), 0).astype(jnp.float32)
    phase_at = (2.0 * math.pi / PHASES) * phase_at + offset[0]
    phases[0] = jnp.cos(phase_at)
    phases[1] = jnp.sin(phase_at)
    phases[2] = jnp.cos(2.0 * phase_at)
    phases[3] = jnp.sin(2.0 * phase_at)
    shift_copy.wait()
    shift_y, shift_x = shift[0:1, 0:1], shift[0:1, 1:2]
    x_cos, x_sin = turn_pair(lax.broadcasted_iota(jnp.int32, (8, PIX), 1) * shift_x)
    row_at = lax.broadcasted_iota(jnp.int32, (ROWS, 128), 0) + rank * ROWS
    y_cos, y_sin = turn_pair(row_at * shift_y)
    x_cos, x_sin = x_cos[:1], x_sin[:1]
    y_cos = jnp.concatenate([y_cos] * 4, axis=1)
    y_sin = jnp.concatenate([y_sin] * 4, axis=1)
    turn_re = x_cos * y_cos - x_sin * y_sin
    turn_im = x_cos * y_sin + x_sin * y_cos
    turns[0] = turn_re
    turns[1] = turn_im
    turns[2] = turn_re * turn_re - turn_im * turn_im
    turns[3] = 2.0 * turn_re * turn_im
    base_copy.wait()
    x_rows(base, 0, (x_hi, x_lo))
    copy.wait()


def spectra_rows(rank, rows, partners, band, x_hi, x_lo, outs):
    table = (
        jnp.concatenate([x_hi[rank ^ k] for k in partners], axis=0),
        jnp.concatenate([x_lo[rank ^ k] for k in partners], axis=0),
    )
    spectra = dot3(table, band, (1, 1))
    for k, out in enumerate(outs):
        for plane in range(5):
            out[plane] = spectra[k * rows : (k + 1) * rows, plane * ROWS : (plane + 1) * ROWS]


def forward_kernel(place, sums0, sums1, sums2, sums3, turns, phases, frames, x_hi, x_lo, *rest):
    outs, (band_hi, band_lo) = rest[:2], rest[2:]
    total = (sums0[...] + sums1[...]) + (sums2[...] + sums3[...])
    weight_all = (PIX * PIX / PHASES) / total
    acc = None
    for p in range(PHASES):
        weight = weight_all[:, p : p + 1]
        plane = frames[p].astype(jnp.float32)
        terms = [plane * weight] + [
            plane * (weight * phases[i, p : p + 1, 0:1]) for i in range(4)
        ]
        acc = terms if p == 0 else [a + b for a, b in zip(acc, terms)]
    zero, one_re, one_im, two_re, two_im = acc
    planes = [
        zero,
        one_re * turns[0] + one_im * turns[1],
        one_re * turns[1] - one_im * turns[0],
        two_re * turns[2] + two_im * turns[3],
        two_re * turns[3] - two_im * turns[2],
    ]
    for index, plane in enumerate(planes):
        hi, lo = split(plane)
        band_hi[index * ROWS : (index + 1) * ROWS, :] = hi
        band_lo[index * ROWS : (index + 1) * ROWS, :] = lo
    band = (band_hi[...], band_lo[...])
    spectra_rows(place[0], 2 * MAIN[0], (2, 3), band, x_hi, x_lo, outs)


def forward_rest_kernel(place, band_hi, band_lo, x_hi0, x_lo0, base, *rest):
    outs, (y_hi, y_lo, x_hi1, x_lo1) = rest[:6], rest[6:]
    x_rows(base, 1, (x_hi1, x_lo1))
    band = (band_hi[...], band_lo[...])
    spectra_rows(place[0], 2 * MAIN[1], (0, 1, 2, 3), band, x_hi1, x_lo1, outs[2:])
    spectra_rows(place[0], 2 * MAIN[0], (0, 1), band, x_hi0, x_lo0, outs[:2])
    for part, out in ((0, y_hi), (1, y_lo)):
        blocks, _ = row_blocks(base, part, PARTS)
        for s in range(PARTS):
            for kind in range(2):
                out[s, kind] = blocks[s][kind].astype(jnp.bfloat16)


def root(value):
    return value * lax.rsqrt(jnp.maximum(value, 1e-30))


def transfer_curve(squared):
    radius = jnp.minimum(root(squared), 1.0)
    arc = jnp.full_like(radius, 2.0 / math.pi * ARC[7])
    for coefficient in ARC[6::-1]:
        arc = arc * radius + 2.0 / math.pi * coefficient
    over = 1.0 + radius
    return root(1.0 - radius) * (arc - (2.0 / math.pi) * radius * (over * lax.rsqrt(over)))


def weights_kernel(chunk, place, gains, shift, after, weights, y_square, y_low):
    rank = place[0]
    shift_y, shift_x = shift[0, 0], shift[0, 1]
    own = [gains[0, m + 2] for m in ORDERS]
    other = [gains[0, 2 - m] for m in ORDERS]
    sub = lax.broadcasted_iota(jnp.int32, (8, 1), 0)
    lane = lax.broadcasted_iota(jnp.int32, (8, PIX), 1)
    for order, m in enumerate(ORDERS):
        y = ((lane - m * shift_y + PIX // 2) & (PIX - 1)) - PIX // 2
        y_low[order] = jnp.where(y + m * shift_y >= 0, 1.0, 0.0)
        y = y.astype(jnp.float32) * (1.0 / (cut_share * PIX))
        y_square[order] = y * y

    def tile_step(tile, carry):
        low = 8 * tile
        folded = low >= MAIN[chunk]
        l = jnp.where(folded, low - MAIN[chunk] + FOLD_LOW[chunk], low + LOW[chunk])
        freq = 64 * (l // 16) + 16 * rank + l % 16
        freq_x = jnp.where(folded, freq - PIX, freq) + sub
        if chunk == 1:
            lone = jnp.logical_and(low == MAIN[1], rank == 0).astype(jnp.int32)
            freq_x = jnp.where(jnp.where(sub == 0, lone, 0) == 1, -PIX // 2, freq_x)
        dens = [jnp.full((8, PIX), wiener, jnp.float32)] * 4
        curves = []
        for order, m in enumerate(ORDERS):
            x = (freq_x - m * shift_x).astype(jnp.float32) * (1.0 / (cut_share * PIX))
            curve = transfer_curve(x * x + y_square[order])
            power = curve * curve
            power_low = power * y_low[order]
            power_high = power - power_low
            g, h = own[order] * own[order], other[order] * other[order]
            dens = [
                dens[0] + g * power_low,
                dens[1] + g * power_high,
                dens[2] + h * power_low,
                dens[3] + h * power_high,
            ]
            curves.append(curve)
        own_low, own_high, other_low, other_high = [0.5 / den for den in dens]
        rows = pl.ds(pl.multiple_of(low, 8), 8)
        for order in range(5):
            is_low = y_low[order] > 0.5
            own_den = jnp.where(is_low, own_low, own_high)
            other_den = jnp.where(is_low, other_low, other_high)
            weight = curves[order] * (own[order] * own_den + other[order] * other_den)
            weights[order, 0, rows, :] = weight
            weights[order, 1, rows, :] = jnp.where(is_low, weight, -weight)

        return carry

    lax.fori_loop(0, COLS[chunk] // 8, tile_step, 0, unroll=2)


def table_kernel(place, first, after, hi0, hi1, lo0, lo1):
    outs = ((hi0, lo0), (hi1, lo1))
    rank = place[0]
    turn = lax.broadcasted_iota(jnp.int32, (8, 128), 0).astype(jnp.float32) * (math.pi / 4)
    turn_re, turn_im = jnp.cos(turn), jnp.sin(turn)
    low = 0
    for chunk in CHUNKS:
        rows = COLS[chunk]
        step_re = jnp.concatenate([turn_re] * (rows // 8), axis=0)
        step_im = jnp.concatenate([turn_im] * (rows // 8), axis=0)
        for k in range(PARTS):
            source = rank ^ k
            re, im = first[source, 0, low : low + rows], first[source, 1, low : low + rows]
            for block in range(GRID // 128):
                lanes = slice(128 * block, 128 * (block + 1))
                for part, value in ((0, re), (1, -im)):
                    at = slice((2 * k + part) * rows, (2 * k + part + 1) * rows)
                    outs[chunk][0][at, lanes], outs[chunk][1][at, lanes] = split(value)
                re, im = re * step_re - im * step_im, re * step_im + im * step_re
        low += rows


def middle_kernel(chunk, place, got0, got1, got2, got3, weights, y_hi, y_lo, odd, *outs):
    rank = place[0]
    blocks = (got0, got1, got2, got3)
    rows, ext, count = COLS[chunk], EXT[chunk], MAIN[chunk]
    if chunk == 1:
        first_row = lax.broadcasted_iota(jnp.int32, (count, PIX), 0) == 0
        lone = jnp.logical_and(first_row, jnp.full((count, PIX), rank, jnp.int32) == 0)
        top = lax.broadcasted_iota(jnp.int32, (8, PIX), 0) == 0
        swap = lone[:8]

    def plane(index):
        whole = jnp.concatenate([b[index] for b in blocks], axis=1)
        cosines, sines = whole[:count], whole[count:]
        if chunk == 0:
            return cosines, sines, None
        return cosines, jnp.where(lone, 0.0, sines), jnp.where(top, sines[:8], 0.0)

    real_rows = []
    imag_rows = []

    def add_row(re, im, extra_re, extra_im):
        real_rows.append(re)
        imag_rows.append(im)
        if chunk == 1:
            real_rows.append(extra_re)
            imag_rows.append(extra_im() if callable(extra_im) else extra_im)

    cos_r, sin_r, extra_r = plane(0)
    add_row(cos_r, -sin_r, extra_r, lambda: jnp.zeros_like(extra_r))
    for m in range(2):
        cos_r, sin_r, extra_r = plane(1 + 2 * m)
        cos_i, sin_i, extra_i = plane(2 + 2 * m)
        add_row(cos_r + sin_i, cos_i - sin_r, extra_r, extra_i)
        add_row(cos_r - sin_i, -cos_i - sin_r, extra_r, lambda: -extra_i)
    data = split(jnp.concatenate(real_rows + imag_rows, axis=0))

    def y_matrix(ref):
        return jnp.concatenate(
            [jnp.concatenate([ref[rank ^ k, 0], ref[rank ^ k, 1]], axis=1) for k in range(PARTS)],
            axis=0,
        )

    turned = dot3(data, (y_matrix(y_hi), y_matrix(y_lo)), (1, 0))
    half = 5 * ext
    spec_re = turned[:half, :PIX] + turned[half:, PIX:]
    spec_im = turned[half:, :PIX] - turned[:half, PIX:]
    sums = None
    for order in range(5):

        def both(spec):
            main = spec[order * ext : order * ext + count]
            if chunk == 0:
                return jnp.concatenate([main, main], axis=0)
            extra = spec[order * ext + count : (order + 1) * ext]
            return jnp.concatenate(
                [main, jnp.where(swap, extra, main[16:24])] + ([main[24:]] if count > 24 else []), axis=0
            )

        re, im = both(spec_re), both(spec_im)
        plus, minus = weights[order, 0], weights[order, 1]
        terms = (plus * re, plus * im, minus * re, minus * im)
        sums = terms if order == 0 else tuple(a + b for a, b in zip(sums, terms))
    even_re, even_im, odd_re, odd_im = sums
    odd_cos, odd_sin = odd[0:1], odd[1:2]
    odd_re, odd_im = odd_re * odd_cos - odd_im * odd_sin, odd_re * odd_sin + odd_im * odd_cos
    filtered = split(jnp.concatenate([even_re, even_im, odd_re, odd_im], axis=0))

    def u_matrix(ref):
        return jnp.concatenate(
            [jnp.concatenate([ref[rank ^ k, 0], ref[rank ^ k, 1]], axis=0) for k in range(PARTS)],
            axis=0,
        )

    back = dot3(filtered, (u_matrix(y_hi), u_matrix(y_lo)), (1, 1))
    for k in range(PARTS):
        cos_part = back[:, 2 * ROWS * k : 2 * ROWS * k + ROWS]
        sin_part = back[:, 2 * ROWS * k + ROWS : 2 * ROWS * (k + 1)]
        for parity in range(2):
            base = 2 * rows * parity
            re, im = slice(base, base + rows), slice(base + rows, base + 2 * rows)
            lanes = slice(parity * ROWS, (parity + 1) * ROWS)
            outs[k][0:rows, lanes] = cos_part[re] - sin_part[im]
            outs[k][rows : 2 * rows, lanes] = sin_part[re] + cos_part[im]


def gathered(blocks):
    return split(jnp.concatenate([b[...] for b in blocks], axis=0).T)


NEAR = 4 * COLS[1]


def part_kernel(got0, got1, got2, got3, near0, near1, hi0, lo0, hi1, lo1, part):
    data = gathered((got0, got1, got2, got3))
    near = gathered((near0, near1))
    part[...] = dot3(data, (hi0[...], lo0[...]), (1, 0)) + dot3(
        near, (hi1[:NEAR], lo1[:NEAR]), (1, 0)
    )


def final_kernel(got2, got3, final_hi, final_lo, part, out, woven, sems):
    data = gathered((got2, got3))
    copies = []
    for strip in range(GRID // 256):
        lanes = slice(256 * strip, 256 * (strip + 1))
        table = (final_hi[NEAR:, lanes], final_lo[NEAR:, lanes])
        picture = part[:, lanes] + dot3(data, table, (1, 0))
        for block in range(2):
            at = 2 * strip + block
            piece = slice(128 * block, 128 * (block + 1))
            woven[at, pl.ds(0, ROWS, 2), :] = picture[:ROWS, piece]
            woven[at, pl.ds(1, ROWS, 2), :] = picture[ROWS:, piece]
            copy = pltpu.make_async_copy(
                woven.at[at], out.at[:, pl.ds(128 * at, 128)], sems.at[at]
            )
            copy.start()
            copies.append(copy)
    for copy in copies:
        copy.wait()


def smem():
    return pl.BlockSpec(memory_space=pltpu.SMEM)


def vmem():
    return pl.BlockSpec(memory_space=pltpu.VMEM)


def hbm():
    return pl.BlockSpec(memory_space=pltpu.HBM)


def f32(*shape):
    return jax.ShapeDtypeStruct(shape, jnp.float32)


def bf16(*shape):
    return jax.ShapeDtypeStruct(shape, jnp.bfloat16)


def call(kernel, out_shape, in_specs, out_specs=None, scratch=(), limit=24):
    if out_specs is None:
        out_specs = jax.tree.map(lambda _: vmem(), out_shape)
    return pl.pallas_call(
        kernel,
        out_shape=out_shape,
        in_specs=in_specs,
        out_specs=out_specs,
        scratch_shapes=list(scratch),
        compiler_params=pltpu.CompilerParams(vmem_limit_bytes=limit * 1024 * 1024),
    )


def from_partners(blocks):
    got = [blocks[0]]
    for k in range(1, PARTS):
        got.append(lax.ppermute(blocks[k], "row", [(i, i ^ k) for i in range(PARTS)]))
    return got


def reconstruct(frames, phase_offset, order_gain, band_shift):
    base, first, odd = tables()
    rank = lax.axis_index("row")
    place = rank.reshape(1).astype(jnp.int32)

    sums = jnp.sum(frames.astype(jnp.float32), axis=(2, 3))
    sums = from_partners([sums] * PARTS)
    table = bf16(PARTS, 2 * MAIN[0], PIX)
    frames, turns, phases, near_base, *x_parts = call(
        phase_kernel,
        [bf16(PHASES, ROWS, PIX), f32(4, ROWS, PIX), f32(4, 8, 128), bf16(*base.shape)]
        + [table] * 2,
        [smem()] * 2 + [hbm()] * 3,
        scratch=[pltpu.VMEM((1, 2), jnp.int32), pltpu.SemaphoreType.DMA((3,))],
    )(
        place,
        phase_offset,
        pltpu.with_memory_space_constraint(band_shift, pltpu.HBM),
        pltpu.with_memory_space_constraint(frames, pltpu.HBM),
        pltpu.with_memory_space_constraint(base, pltpu.HBM),
    )
    blocks = [f32(5, 2 * MAIN[c], ROWS) for c in CHUNKS]
    *far, band_hi, band_lo = call(
        forward_kernel,
        [blocks[0]] * 2 + [bf16(5 * ROWS, PIX)] * 2,
        [smem()] + [vmem()] * 9,
    )(place, *sums, turns, phases, frames, *x_parts)
    *sent, y_hi, y_lo = call(
        forward_rest_kernel,
        [blocks[0]] * 2 + [blocks[1]] * PARTS + [bf16(PARTS, 2, ROWS, PIX)] * 2,
        [smem()] + [vmem()] * 5,
        scratch=[pltpu.VMEM((PARTS, 2 * MAIN[1], PIX), jnp.bfloat16)] * 2,
    )(place, band_hi, band_lo, *x_parts, near_base)
    spectra = [from_partners([*sent[:2], *far]), from_partners(sent[2:])]
    got = []
    after = sent[0]
    for c in CHUNKS:
        weights = call(
            functools.partial(weights_kernel, c),
            f32(5, 2, COLS[c], PIX),
            [smem()] * 3 + [vmem()],
            scratch=[pltpu.VMEM((5, 8, PIX), jnp.float32)] * 2,
        )(place, order_gain, band_shift, after)
        sent = call(
            functools.partial(middle_kernel, c),
            [f32(2 * COLS[c], 2 * ROWS)] * PARTS,
            [smem()] + [vmem()] * 8,
        )(place, *spectra[c], weights, y_hi, y_lo, odd)
        after = sent[0]
        got.append(from_partners(sent))
    hi0, hi1, lo0, lo1 = call(
        table_kernel,
        [bf16(8 * COLS[c], GRID) for c in CHUNKS] * 2,
        [smem()] + [vmem()] * 2,
    )(place, first, after)
    part = call(part_kernel, f32(2 * ROWS, GRID), [vmem()] * 10)(
        *got[0], *got[1][:2], hi0, lo0, hi1, lo1
    )
    return call(
        final_kernel,
        f32(2 * ROWS, GRID),
        [vmem()] * 5,
        hbm(),
        [
            pltpu.VMEM((GRID // 128, 2 * ROWS, 128), jnp.float32),
            pltpu.SemaphoreType.DMA((GRID // 128,)),
        ],
    )(*got[1][2:], hi1, lo1, part)


def solution(mesh):
    in_specs = (P("fov", None, "row", None), P("fov"), P("fov", None), P("fov", None))
    out_specs = P(("fov", "row"), None)
    return jax.shard_map(
        reconstruct, mesh=mesh, in_specs=in_specs, out_specs=out_specs, check_vma=False
    )
```

```python
import functools
import math

import jax
import jax.numpy as jnp
import numpy as np
from jax import lax
from jax.experimental import pallas as pl
from jax.experimental.pallas import tpu as pltpu
from jax.sharding import PartitionSpec as P


wiener = 0.1
gain_out = 8.0
cut_share = 0.45
PIX = 512
GRID = 1024
PHASES = 5
PARTS = 4
ROWS = PIX // PARTS
CHUNKS = (0, 1)
LOW = (32, 0)
MAIN = (32, 32)
FOLD_LOW = (32, 16)
FOLD = (32, 16)
COLS = (64, 48)
EXT = (32, 40)
ORDERS = (0, 1, -1, 2, -2)
ARC = (
    1.5707963050,
    -0.2145988016,
    0.0889789874,
    -0.0501743046,
    0.0308918810,
    -0.0170881256,
    0.0066700901,
    -0.0012624911,
)


def split_np(array):
    hi = array.astype(jnp.bfloat16)
    lo = (array - hi.astype(np.float32)).astype(jnp.bfloat16)
    return hi, lo


def split(array):
    hi = array.astype(jnp.bfloat16)
    lo = (array - hi.astype(jnp.float32)).astype(jnp.bfloat16)
    return hi, lo


def column_freq_np(d, chunk):
    def column(low, count):
        l = np.arange(low, low + count)
        return 64 * (l // 16) + 16 * d + l % 16

    fold = column(FOLD_LOW[chunk], FOLD[chunk]) - PIX
    if d == 0 and chunk == 1:
        fold[0] = -PIX // 2
    return np.concatenate([column(LOW[chunk], MAIN[chunk]), fold])


@functools.cache
def tables():
    index = np.arange(PIX)
    angle = 2.0 * np.pi * (np.outer(index[:ROWS], index) % PIX) / PIX
    base = np.stack([np.cos(angle), np.sin(angle)]).astype(np.float32)
    first = np.zeros((PARTS, 2, sum(COLS), 128), np.float32)
    for s in range(PARTS):
        freq = np.concatenate([column_freq_np(s, c) for c in CHUNKS])
        scale = gain_out / (GRID * GRID) * np.where(freq == 0, 1.0, 2.0)
        turn = 2.0 * np.pi * ((freq[:, None] * np.arange(128)[None, :]) % GRID) / GRID
        first[s, 0] = scale[:, None] * np.cos(turn)
        first[s, 1] = scale[:, None] * np.sin(turn)
    turn = 2.0 * np.pi * index / GRID
    odd = np.stack([np.cos(turn), np.sin(turn)]).astype(np.float32)
    return np.stack(split_np(base)), first, odd


def dot3(left, right, dims):
    lhs = jnp.concatenate([left[0], left[0], left[1]], axis=dims[0])
    rhs = jnp.concatenate([right[0], right[1], right[0]], axis=dims[1])
    return lax.dot_general(
        lhs, rhs, (((dims[0],), (dims[1],)), ((), ())), preferred_element_type=jnp.float32
    )


def turn_pair(steps):
    angle = (2.0 * math.pi / PIX) * ((steps + 256) % 512 - 256).astype(jnp.float32)
    return jnp.cos(angle), jnp.sin(angle)


def row_blocks(base, part, count):
    lane = lax.broadcasted_iota(jnp.int32, (1, PIX), 1)
    parity = lane % 2
    sign = (1 - lane % 4 + parity).astype(jnp.float32)
    quarter_re = jnp.where(parity == 0, sign, 0.0)
    quarter_im = jnp.where(parity == 1, sign, 0.0)
    half_turn = 1.0 - 2.0 * parity.astype(jnp.float32)
    cosine, sine = base[part, 0].astype(jnp.float32), base[part, 1].astype(jnp.float32)
    cos_re, cos_im = cosine * quarter_re, cosine * quarter_im
    sin_re, sin_im = sine * quarter_re, sine * quarter_im
    blocks = [(cosine, sine), (cos_re - sin_im, sin_re + cos_im)]
    if count > 2:
        blocks += [
            (cosine * half_turn, sine * half_turn),
            (cos_re + sin_im, sin_re - cos_im),
        ]
    return blocks, half_turn


def x_rows(base, chunk, outs):
    top = lax.broadcasted_iota(jnp.int32, (8, PIX), 0) == 0
    for part in range(2):
        blocks, half_turn = row_blocks(base, part, 2)
        lone = half_turn if part == 0 else jnp.zeros_like(half_turn)
        for d in range(PARTS):
            pieces = []
            for kind in range(2):
                for l in range(LOW[chunk], LOW[chunk] + MAIN[chunk], 8):
                    column = 64 * (l // 16) + 16 * d + l % 16
                    s, t = column // ROWS, column % ROWS
                    piece = blocks[s][kind][t : t + 8]
                    if column == 0 and kind == 1:
                        piece = jnp.where(top, lone, piece)
                    pieces.append(piece)
            outs[part][d] = jnp.concatenate(pieces, axis=0).astype(jnp.bfloat16)


def phase_kernel(
    place, offset, shift_far, source, base_far, frames, turns, phases, base, x_hi, x_lo, shift, sems
):
    base_copy = pltpu.make_async_copy(base_far, base, sems.at[0])
    base_copy.start()
    shift_copy = pltpu.make_async_copy(shift_far, shift, sems.at[1])
    shift_copy.start()
    copy = pltpu.make_async_copy(source.at[0], frames, sems.at[2])
    copy.start()
    rank = place[0]
    phase_at = lax.broadcasted_iota(jnp.int32, (8, 128), 0).astype(jnp.float32)
    phase_at = (2.0 * math.pi / PHASES) * phase_at + offset[0]
    phases[0] = jnp.cos(phase_at)
    phases[1] = jnp.sin(phase_at)
    phases[2] = jnp.cos(2.0 * phase_at)
    phases[3] = jnp.sin(2.0 * phase_at)
    shift_copy.wait()
    shift_y, shift_x = shift[0:1, 0:1], shift[0:1, 1:2]
    x_cos, x_sin = turn_pair(lax.broadcasted_iota(jnp.int32, (8, PIX), 1) * shift_x)
    row_at = lax.broadcasted_iota(jnp.int32, (ROWS, 128), 0) + rank * ROWS
    y_cos, y_sin = turn_pair(row_at * shift_y)
    x_cos, x_sin = x_cos[:1], x_sin[:1]
    y_cos = jnp.concatenate([y_cos] * 4, axis=1)
    y_sin = jnp.concatenate([y_sin] * 4, axis=1)
    turn_re = x_cos * y_cos - x_sin * y_sin
    turn_im = x_cos * y_sin + x_sin * y_cos
    turns[0] = turn_re
    turns[1] = turn_im
    turns[2] = turn_re * turn_re - turn_im * turn_im
    turns[3] = 2.0 * turn_re * turn_im
    base_copy.wait()
    x_rows(base, 0, (x_hi, x_lo))
    copy.wait()


def spectra_rows(rank, rows, partners, band, x_hi, x_lo, outs):
    table = (
        jnp.concatenate([x_hi[rank ^ k] for k in partners], axis=0),
        jnp.concatenate([x_lo[rank ^ k] for k in partners], axis=0),
    )
    spectra = dot3(table, band, (1, 1))
    for k, out in enumerate(outs):
        for plane in range(5):
            out[plane] = spectra[k * rows : (k + 1) * rows, plane * ROWS : (plane + 1) * ROWS]


def forward_kernel(place, sums0, sums1, sums2, sums3, turns, phases, frames, x_hi, x_lo, *rest):
    outs, (band_hi, band_lo) = rest[:2], rest[2:]
    total = (sums0[...] + sums1[...]) + (sums2[...] + sums3[...])
    weight_all = (PIX * PIX / PHASES) / total
    acc = None
    for p in range(PHASES):
        weight = weight_all[:, p : p + 1]
        plane = frames[p].astype(jnp.float32)
        terms = [plane * weight] + [
            plane * (weight * phases[i, p : p + 1, 0:1]) for i in range(4)
        ]
        acc = terms if p == 0 else [a + b for a, b in zip(acc, terms)]
    zero, one_re, one_im, two_re, two_im = acc
    planes = [
        zero,
        one_re * turns[0] + one_im * turns[1],
        one_re * turns[1] - one_im * turns[0],
        two_re * turns[2] + two_im * turns[3],
        two_re * turns[3] - two_im * turns[2],
    ]
    for index, plane in enumerate(planes):
        hi, lo = split(plane)
        band_hi[index * ROWS : (index + 1) * ROWS, :] = hi
        band_lo[index * ROWS : (index + 1) * ROWS, :] = lo
    band = (band_hi[...], band_lo[...])
    spectra_rows(place[0], 2 * MAIN[0], (2, 3), band, x_hi, x_lo, outs)


def forward_rest_kernel(place, band_hi, band_lo, x_hi0, x_lo0, base, *rest):
    outs, (y_hi, y_lo, x_hi1, x_lo1) = rest[:6], rest[6:]
    x_rows(base, 1, (x_hi1, x_lo1))
    band = (band_hi[...], band_lo[...])
    spectra_rows(place[0], 2 * MAIN[1], (0, 1, 2, 3), band, x_hi1, x_lo1, outs[2:])
    spectra_rows(place[0], 2 * MAIN[0], (0, 1), band, x_hi0, x_lo0, outs[:2])
    for part, out in ((0, y_hi), (1, y_lo)):
        blocks, _ = row_blocks(base, part, PARTS)
        for s in range(PARTS):
            for kind in range(2):
                out[s, kind] = blocks[s][kind].astype(jnp.bfloat16)


def root(value):
    return value * lax.rsqrt(jnp.maximum(value, 1e-30))


def transfer_curve(squared):
    radius = jnp.minimum(root(squared), 1.0)
    arc = jnp.full_like(radius, 2.0 / math.pi * ARC[7])
    for coefficient in ARC[6::-1]:
        arc = arc * radius + 2.0 / math.pi * coefficient
    over = 1.0 + radius
    return root(1.0 - radius) * (arc - (2.0 / math.pi) * radius * (over * lax.rsqrt(over)))


def weights_kernel(chunk, place, gains, shift, after, weights, y_square, y_low):
    rank = place[0]
    shift_y, shift_x = shift[0, 0], shift[0, 1]
    own = [gains[0, m + 2] for m in ORDERS]
    other = [gains[0, 2 - m] for m in ORDERS]
    sub = lax.broadcasted_iota(jnp.int32, (8, 1), 0)
    lane = lax.broadcasted_iota(jnp.int32, (8, PIX), 1)
    for order, m in enumerate(ORDERS):
        y = ((lane - m * shift_y + PIX // 2) & (PIX - 1)) - PIX // 2
        y_low[order] = jnp.where(y + m * shift_y >= 0, 1.0, 0.0)
        y = y.astype(jnp.float32) * (1.0 / (cut_share * PIX))
        y_square[order] = y * y

    def tile_step(tile, carry):
        low = 8 * tile
        folded = low >= MAIN[chunk]
        l = jnp.where(folded, low - MAIN[chunk] + FOLD_LOW[chunk], low + LOW[chunk])
        freq = 64 * (l // 16) + 16 * rank + l % 16
        freq_x = jnp.where(folded, freq - PIX, freq) + sub
        if chunk == 1:
            lone = jnp.logical_and(low == MAIN[1], rank == 0).astype(jnp.int32)
            freq_x = jnp.where(jnp.where(sub == 0, lone, 0) == 1, -PIX // 2, freq_x)
        dens = [jnp.full((8, PIX), wiener, jnp.float32)] * 4
        curves = []
        for order, m in enumerate(ORDERS):
            x = (freq_x - m * shift_x).astype(jnp.float32) * (1.0 / (cut_share * PIX))
            curve = transfer_curve(x * x + y_square[order])
            power = curve * curve
            power_low = power * y_low[order]
            power_high = power - power_low
            g, h = own[order] * own[order], other[order] * other[order]
            dens = [
                dens[0] + g * power_low,
                dens[1] + g * power_high,
                dens[2] + h * power_low,
                dens[3] + h * power_high,
            ]
            curves.append(curve)
        own_low, own_high, other_low, other_high = [0.5 / den for den in dens]
        rows = pl.ds(pl.multiple_of(low, 8), 8)
        for order in range(5):
            is_low = y_low[order] > 0.5
            own_den = jnp.where(is_low, own_low, own_high)
            other_den = jnp.where(is_low, other_low, other_high)
            weight = curves[order] * (own[order] * own_den + other[order] * other_den)
            weights[order, 0, rows, :] = weight
            weights[order, 1, rows, :] = jnp.where(is_low, weight, -weight)

        return carry

    lax.fori_loop(0, COLS[chunk] // 8, tile_step, 0, unroll=4 - chunk)


def table_kernel(place, first, after, hi0, hi1, lo0, lo1):
    outs = ((hi0, lo0), (hi1, lo1))
    rank = place[0]
    turn = lax.broadcasted_iota(jnp.int32, (8, 128), 0).astype(jnp.float32) * (math.pi / 4)
    turn_re, turn_im = jnp.cos(turn), jnp.sin(turn)
    low = 0
    for chunk in CHUNKS:
        rows = COLS[chunk]
        step_re = jnp.concatenate([turn_re] * (rows // 8), axis=0)
        step_im = jnp.concatenate([turn_im] * (rows // 8), axis=0)
        for k in range(PARTS):
            source = rank ^ k
            re, im = first[source, 0, low : low + rows], first[source, 1, low : low + rows]
            for block in range(GRID // 128):
                lanes = slice(128 * block, 128 * (block + 1))
                for part, value in ((0, re), (1, -im)):
                    at = slice((2 * k + part) * rows, (2 * k + part + 1) * rows)
                    outs[chunk][0][at, lanes], outs[chunk][1][at, lanes] = split(value)
                re, im = re * step_re - im * step_im, re * step_im + im * step_re
        low += rows


def middle_kernel(chunk, place, got0, got1, got2, got3, weights, y_hi, y_lo, odd, *outs):
    rank = place[0]
    blocks = (got0, got1, got2, got3)
    rows, ext, count = COLS[chunk], EXT[chunk], MAIN[chunk]
    if chunk == 1:
        first_row = lax.broadcasted_iota(jnp.int32, (count, PIX), 0) == 0
        lone = jnp.logical_and(first_row, jnp.full((count, PIX), rank, jnp.int32) == 0)
        top = lax.broadcasted_iota(jnp.int32, (8, PIX), 0) == 0
        swap = lone[:8]

    def plane(index):
        whole = jnp.concatenate([b[index] for b in blocks], axis=1)
        cosines, sines = whole[:count], whole[count:]
        if chunk == 0:
            return cosines, sines, None
        return cosines, jnp.where(lone, 0.0, sines), jnp.where(top, sines[:8], 0.0)

    real_rows = []
    imag_rows = []

    def add_row(re, im, extra_re, extra_im):
        real_rows.append(re)
        imag_rows.append(im)
        if chunk == 1:
            real_rows.append(extra_re)
            imag_rows.append(extra_im() if callable(extra_im) else extra_im)

    cos_r, sin_r, extra_r = plane(0)
    add_row(cos_r, -sin_r, extra_r, lambda: jnp.zeros_like(extra_r))
    for m in range(2):
        cos_r, sin_r, extra_r = plane(1 + 2 * m)
        cos_i, sin_i, extra_i = plane(2 + 2 * m)
        add_row(cos_r + sin_i, cos_i - sin_r, extra_r, extra_i)
        add_row(cos_r - sin_i, -cos_i - sin_r, extra_r, lambda: -extra_i)
    data = split(jnp.concatenate(real_rows + imag_rows, axis=0))

    def y_matrix(ref):
        return jnp.concatenate(
            [jnp.concatenate([ref[rank ^ k, 0], ref[rank ^ k, 1]], axis=1) for k in range(PARTS)],
            axis=0,
        )

    turned = dot3(data, (y_matrix(y_hi), y_matrix(y_lo)), (1, 0))
    half = 5 * ext
    spec_re = turned[:half, :PIX] + turned[half:, PIX:]
    spec_im = turned[half:, :PIX] - turned[:half, PIX:]
    sums = None
    for order in range(5):

        def both(spec):
            main = spec[order * ext : order * ext + count]
            if chunk == 0:
                return jnp.concatenate([main, main], axis=0)
            extra = spec[order * ext + count : (order + 1) * ext]
            return jnp.concatenate(
                [main, jnp.where(swap, extra, main[16:24])] + ([main[24:]] if count > 24 else []), axis=0
            )

        re, im = both(spec_re), both(spec_im)
        plus, minus = weights[order, 0], weights[order, 1]
        terms = (plus * re, plus * im, minus * re, minus * im)
        sums = terms if order == 0 else tuple(a + b for a, b in zip(sums, terms))
    even_re, even_im, odd_re, odd_im = sums
    odd_cos, odd_sin = odd[0:1], odd[1:2]
    odd_re, odd_im = odd_re * odd_cos - odd_im * odd_sin, odd_re * odd_sin + odd_im * odd_cos
    filtered = split(jnp.concatenate([even_re, even_im, odd_re, odd_im], axis=0))

    def u_matrix(ref):
        return jnp.concatenate(
            [jnp.concatenate([ref[rank ^ k, 0], ref[rank ^ k, 1]], axis=0) for k in range(PARTS)],
            axis=0,
        )

    back = dot3(filtered, (u_matrix(y_hi), u_matrix(y_lo)), (1, 1))
    for k in range(PARTS):
        cos_part = back[:, 2 * ROWS * k : 2 * ROWS * k + ROWS]
        sin_part = back[:, 2 * ROWS * k + ROWS : 2 * ROWS * (k + 1)]
        for parity in range(2):
            base = 2 * rows * parity
            re, im = slice(base, base + rows), slice(base + rows, base + 2 * rows)
            lanes = slice(parity * ROWS, (parity + 1) * ROWS)
            outs[k][0:rows, lanes] = cos_part[re] - sin_part[im]
            outs[k][rows : 2 * rows, lanes] = sin_part[re] + cos_part[im]


def gathered(blocks):
    return split(jnp.concatenate([b[...] for b in blocks], axis=0).T)


NEAR = 4 * COLS[1]


def part_kernel(got0, got1, got2, got3, near0, near1, hi0, lo0, hi1, lo1, part):
    data = gathered((got0, got1, got2, got3))
    near = gathered((near0, near1))
    part[...] = dot3(data, (hi0[...], lo0[...]), (1, 0)) + dot3(
        near, (hi1[:NEAR], lo1[:NEAR]), (1, 0)
    )


def final_kernel(got2, got3, final_hi, final_lo, part, out, woven, sems):
    data = gathered((got2, got3))
    copies = []
    for strip in range(GRID // 256):
        lanes = slice(256 * strip, 256 * (strip + 1))
        table = (final_hi[NEAR:, lanes], final_lo[NEAR:, lanes])
        picture = part[:, lanes] + dot3(data, table, (1, 0))
        for block in range(2):
            at = 2 * strip + block
            piece = slice(128 * block, 128 * (block + 1))
            woven[at, pl.ds(0, ROWS, 2), :] = picture[:ROWS, piece]
            woven[at, pl.ds(1, ROWS, 2), :] = picture[ROWS:, piece]
            copy = pltpu.make_async_copy(
                woven.at[at], out.at[:, pl.ds(128 * at, 128)], sems.at[at]
            )
            copy.start()
            copies.append(copy)
    for copy in copies:
        copy.wait()


def smem():
    return pl.BlockSpec(memory_space=pltpu.SMEM)


def vmem():
    return pl.BlockSpec(memory_space=pltpu.VMEM)


def hbm():
    return pl.BlockSpec(memory_space=pltpu.HBM)


def f32(*shape):
    return jax.ShapeDtypeStruct(shape, jnp.float32)


def bf16(*shape):
    return jax.ShapeDtypeStruct(shape, jnp.bfloat16)


def call(kernel, out_shape, in_specs, out_specs=None, scratch=(), limit=24):
    if out_specs is None:
        out_specs = jax.tree.map(lambda _: vmem(), out_shape)
    return pl.pallas_call(
        kernel,
        out_shape=out_shape,
        in_specs=in_specs,
        out_specs=out_specs,
        scratch_shapes=list(scratch),
        compiler_params=pltpu.CompilerParams(vmem_limit_bytes=limit * 1024 * 1024),
    )


def from_partners(blocks):
    got = [blocks[0]]
    for k in range(1, PARTS):
        got.append(lax.ppermute(blocks[k], "row", [(i, i ^ k) for i in range(PARTS)]))
    return got


def reconstruct(frames, phase_offset, order_gain, band_shift):
    base, first, odd = tables()
    rank = lax.axis_index("row")
    place = rank.reshape(1).astype(jnp.int32)

    sums = jnp.sum(frames.astype(jnp.float32), axis=(2, 3))
    sums = from_partners([sums] * PARTS)
    table = bf16(PARTS, 2 * MAIN[0], PIX)
    frames, turns, phases, near_base, *x_parts = call(
        phase_kernel,
        [bf16(PHASES, ROWS, PIX), f32(4, ROWS, PIX), f32(4, 8, 128), bf16(*base.shape)]
        + [table] * 2,
        [smem()] * 2 + [hbm()] * 3,
        scratch=[pltpu.VMEM((1, 2), jnp.int32), pltpu.SemaphoreType.DMA((3,))],
    )(
        place,
        phase_offset,
        pltpu.with_memory_space_constraint(band_shift, pltpu.HBM),
        pltpu.with_memory_space_constraint(frames, pltpu.HBM),
        pltpu.with_memory_space_constraint(base, pltpu.HBM),
    )
    blocks = [f32(5, 2 * MAIN[c], ROWS) for c in CHUNKS]
    *far, band_hi, band_lo = call(
        forward_kernel,
        [blocks[0]] * 2 + [bf16(5 * ROWS, PIX)] * 2,
        [smem()] + [vmem()] * 9,
    )(place, *sums, turns, phases, frames, *x_parts)
    *sent, y_hi, y_lo = call(
        forward_rest_kernel,
        [blocks[0]] * 2 + [blocks[1]] * PARTS + [bf16(PARTS, 2, ROWS, PIX)] * 2,
        [smem()] + [vmem()] * 5,
        scratch=[pltpu.VMEM((PARTS, 2 * MAIN[1], PIX), jnp.bfloat16)] * 2,
    )(place, band_hi, band_lo, *x_parts, near_base)
    spectra = [from_partners([*sent[:2], *far]), from_partners(sent[2:])]
    got = []
    after = sent[0]
    for c in CHUNKS:
        weights = call(
            functools.partial(weights_kernel, c),
            f32(5, 2, COLS[c], PIX),
            [smem()] * 3 + [vmem()],
            scratch=[pltpu.VMEM((5, 8, PIX), jnp.float32)] * 2,
        )(place, order_gain, band_shift, after)
        sent = call(
            functools.partial(middle_kernel, c),
            [f32(2 * COLS[c], 2 * ROWS)] * PARTS,
            [smem()] + [vmem()] * 8,
        )(place, *spectra[c], weights, y_hi, y_lo, odd)
        after = sent[0]
        got.append(from_partners(sent))
    hi0, hi1, lo0, lo1 = call(
        table_kernel,
        [bf16(8 * COLS[c], GRID) for c in CHUNKS] * 2,
        [smem()] + [vmem()] * 2,
    )(place, first, after)
    part = call(part_kernel, f32(2 * ROWS, GRID), [vmem()] * 10)(
        *got[0], *got[1][:2], hi0, lo0, hi1, lo1
    )
    return call(
        final_kernel,
        f32(2 * ROWS, GRID),
        [vmem()] * 5,
        hbm(),
        [
            pltpu.VMEM((GRID // 128, 2 * ROWS, 128), jnp.float32),
            pltpu.SemaphoreType.DMA((GRID // 128,)),
        ],
    )(*got[1][2:], hi1, lo1, part)


def solution(mesh):
    in_specs = (P("fov", None, "row", None), P("fov"), P("fov", None), P("fov", None))
    out_specs = P(("fov", "row"), None)
    return jax.shard_map(
        reconstruct, mesh=mesh, in_specs=in_specs, out_specs=out_specs, check_vma=False
    )
```
